256 devices in a mesh: win: 4 (over z_hi), slab: 64 (over y, x, z_lo, core).
Axes of the slice: x: 4, y: 4, z: 8 (z_hi: 4, z_lo: 2; z = z_hi * 2 + z_lo), core: 2. Of those that a mesh axis runs over, the one named last changes fastest.
Arguments:
- lambdas: float32 [16], P('win'), parts along dimension 0, may hold values from 0 to 1
- charge_a: float32 [16, 32768], P('win', 'slab'), parts along dimension 0, may hold values from -3 to 3
- charge_b: float32 [16, 32768], P('win', 'slab'), parts along dimension 0, may hold values from -3 to 3
- perturbed: int32 [16, 32768], P('win', 'slab'), parts along dimension 0, may hold values 0 or 1
- grid_index: int32 [3, 16, 32768], P(None, 'win', 'slab'), parts along dimension 1, may hold values from 0 to 127, as said below
- spline_weights: float32 [3, 4, 16, 32768], P(None, None, 'win', 'slab'), parts along dimension 2, may hold values from 0 to 1, as said below
- spline_slopes: float32 [3, 4, 16, 32768], P(None, None, 'win', 'slab'), parts along dimension 2, may hold values from -1 to 1, as said below
Outputs:
- forces: float32 [3, 16, 32768], P(None, 'win', 'slab'), parts along dimension 1
- energy: float32 [16], P('win'), parts along dimension 0
- lambda_slope: float32 [16], P('win'), parts along dimension 0
The draws below stay inside these ranges and needn't reach their ends.
There are 4 independent parts, one for each index of `win`. The reference program is written for one: setup_inputs(seed, part) draws one part's arguments, and reference() takes and returns one part's arrays. A program takes and returns all parts, laid end to end along the dimension named above; each array names one. Nothing has to cross between parts.
Inputs may be any that keep to these rules, and one draw needn't show every extreme that they name: `grid_index`: the z index of atom i lies in the planes of the slab index that holds it: from (i // 512) * 2 to that plus 2 - 1. `spline_weights`: along each dimension the four weights are the cubic B-spline values (1-u)^3/6, (3u^3-6u^2+4)/6, (-3u^3+3u^2+3u+1)/6, u^3/6 of the atom's fractional offset u in [0, 1). `spline_slopes`: the derivatives in u of spline_weights at the same offsets.
All inputs are finite; a program needn't handle non-finite values. No bound on the sum of `perturbed` on one device may be relied on, other than what follows from the above.
Results may differ from the reference program's by a relative error of at most 0.0003.
Values sent between devices are 32-bit elements; how exact they have to be, the bound alone decides.
No kernel may reach another device: no remote copies, remote signals or barrier semaphores. Data moves between devices by JAX's collectives and lax.ppermute only.
A program may use at most 64 MiB of HBM per device.

```python
import math
import jax
import jax.numpy as jnp

NX = 128
NY = 128
NZ = 128
WINS = 4
ATOM_DEV = 512
ATOMS = 32768
SLAB_Z = 2


def spline_parts(key):
    fraction = jax.random.uniform(jax.random.fold_in(key, 17), (3, WINS, ATOMS), jnp.float32)
    remain = 1.0 - fraction
    weights = jnp.stack([remain ** 3 / 6.0, (3.0 * fraction ** 3 - 6.0 * fraction ** 2 + 4.0) / 6.0, (-3.0 * fraction ** 3 + 3.0 * fraction ** 2 + 3.0 * fraction + 1.0) / 6.0, fraction ** 3 / 6.0], axis=1)
    slopes = jnp.stack([-remain ** 2 / 2.0, (3.0 * fraction ** 2 - 4.0 * fraction) / 2.0, (-3.0 * fraction ** 2 + 2.0 * fraction + 1.0) / 2.0, fraction ** 2 / 2.0], axis=1)
    return (weights, slopes)


def draw_spline_weights(key, part):
    return spline_parts(key)[0].astype(jnp.float32)


def draw_spline_slopes(key, part):
    return spline_parts(key)[1].astype(jnp.float32)


def draw_grid_index(key, part):
    subkeys = jax.random.split(jax.random.fold_in(key, 5), 3)
    column = jax.random.randint(subkeys[0], (WINS, ATOMS), 0, NX)
    row_cell = jax.random.randint(subkeys[1], (WINS, ATOMS), 0, NY)
    owners = jnp.arange(ATOMS, dtype=jnp.int32) // ATOM_DEV
    depths = owners[None, :] * SLAB_Z + jax.random.randint(subkeys[2], (WINS, ATOMS), 0, SLAB_Z)
    return jnp.stack([column, row_cell, depths]).astype(jnp.int32)


def touch_ends(drawn, own_key, smallest, largest):
    longest = drawn.shape.index(max(drawn.shape))
    spots = []
    for shift in (0, 1):
        where = [jax.random.randint(jax.random.fold_in(own_key, axis), (), 0, length) for axis, length in enumerate(drawn.shape)]
        where[longest] = (where[longest] + shift) % drawn.shape[longest]
        spots.append(tuple(where))
    return drawn.at[spots[0]].set(smallest).at[spots[1]].set(largest)


def steps_of(own_key, dims, pieces, smallest, top_value):
    loudness, own = 1.0, jax.random.fold_in(own_key, 6)
    for position, parts in pieces:
        heights = jnp.exp(jax.random.uniform(jax.random.fold_in(own, position), (parts,), jnp.float32, smallest / len(pieces), top_value / len(pieces)))
        loudness = loudness * jnp.repeat(heights, dims[position] // parts).reshape([-1 if axis == position else 1 for axis in range(len(dims))])
    return loudness


def bell_draw(rng, extent, spread, reach, shards=(), held_as=jnp.bfloat16):
    entries = spread * jax.random.normal(rng, extent, jnp.float32)
    if shards:
        entries = entries * steps_of(rng, extent, shards, -0.22, 0.18)
    return jnp.clip(entries, -reach, reach).astype(held_as)


def setup_inputs(seed: int = 0, part: int = 0) -> dict:
    seeds = jax.random.split(jax.random.key(seed), 8)
    part_splits = jax.random.split(jax.random.fold_in(seeds[7], part), 8)
    return {
        "lambdas": jnp.clip(jax.random.uniform(part_splits[0], (WINS,), jnp.float32, 0.0, 1.0), 0.0, 1.0),
        "charge_a": bell_draw(part_splits[1], (WINS, ATOMS), 0.5, 3.0, ((1, 64),), jnp.float32),
        "charge_b": bell_draw(part_splits[2], (WINS, ATOMS), 0.5, 3.0, ((1, 64),), jnp.float32),
        "perturbed": touch_ends((jax.random.randint(part_splits[3], (WINS, ATOMS), 0, 4) < 1).astype(jnp.int32), jax.random.fold_in(part_splits[3], 1), 0, 1),
        "grid_index": draw_grid_index(jax.random.fold_in(jax.random.fold_in(seeds[7], part), 71), part),
        "spline_weights": draw_spline_weights(jax.random.fold_in(jax.random.fold_in(seeds[7], part), 71), part),
        "spline_slopes": draw_spline_slopes(jax.random.fold_in(jax.random.fold_in(seeds[7], part), 71), part),
    }


gauss_width = 2.0


def frequency(length):
    counter = jnp.arange(length, dtype=jnp.int32)
    return jnp.where(counter >= length // 2, counter - length, counter).astype(jnp.float32) / length


def influence_table():
    along_z = frequency(NZ)[:, None, None]
    along_x = frequency(NX)[None, :, None]
    along_y = frequency(NY)[None, None, :]
    squared = along_z * along_z + along_x * along_x + along_y * along_y
    positive = squared > 0
    safe_value = jnp.where(positive, squared, jnp.float32(1.0))
    return jnp.where(positive, jnp.exp(-gauss_width * squared) / (math.pi * NX * NY * NZ * safe_value), jnp.float32(0.0))


def reference(lambdas, charge_a, charge_b, perturbed, grid_index, spline_weights, spline_slopes):
    influence = influence_table()
    offsets = jnp.arange(4, dtype=jnp.int32)
    force_list = []
    energy_list = []
    slope_list = []
    for window in range(WINS):
        flag_values = perturbed[window].astype(jnp.float32)
        charge = charge_a[window] + flag_values * lambdas[window] * (charge_b[window] - charge_a[window])
        charge_step = flag_values * (charge_b[window] - charge_a[window])
        cells_z = ((grid_index[2, window][:, None] + offsets[None, :]) % NZ)[:, :, None, None]
        cells_x = ((grid_index[0, window][:, None] + offsets[None, :]) % NX)[:, None, :, None]
        cells_y = ((grid_index[1, window][:, None] + offsets[None, :]) % NY)[:, None, None, :]
        weight_z = spline_weights[2, :, window].T[:, :, None, None]
        weight_x = spline_weights[0, :, window].T[:, None, :, None]
        weight_y = spline_weights[1, :, window].T[:, None, None, :]
        slope_z = spline_slopes[2, :, window].T[:, :, None, None]
        slope_x = spline_slopes[0, :, window].T[:, None, :, None]
        slope_y = spline_slopes[1, :, window].T[:, None, None, :]
        stencil = weight_z * weight_x * weight_y
        charge_grid = jnp.zeros((NZ, NX, NY), jnp.float32).at[cells_z, cells_x, cells_y].add(charge[:, None, None, None] * stencil)
        spectrum = jnp.fft.fftn(charge_grid)
        power_map = jnp.real(spectrum) ** 2 + jnp.imag(spectrum) ** 2
        energy_list.append(0.5 * jnp.sum(influence * power_map))
        potential = jnp.real(jnp.fft.ifftn(influence * spectrum)) * (NX * NY * NZ)
        sampled = potential[cells_z, cells_x, cells_y]
        atom_value = jnp.sum(stencil * sampled, axis=(1, 2, 3))
        force_x = -charge * jnp.sum(weight_z * slope_x * weight_y * sampled, axis=(1, 2, 3))
        force_y = -charge * jnp.sum(weight_z * weight_x * slope_y * sampled, axis=(1, 2, 3))
        force_z = -charge * jnp.sum(slope_z * weight_x * weight_y * sampled, axis=(1, 2, 3))
        force_list.append(jnp.stack([force_x, force_y, force_z]))
        slope_list.append(jnp.sum(charge_step * atom_value))
    forces = jnp.stack(force_list, axis=1)
    energy = jnp.stack(energy_list) / ATOMS
    lambda_slope = jnp.stack(slope_list) / ATOMS
    return (forces, energy, lambda_slope)
```

```python
import math

import jax
import jax.numpy as jnp
import numpy as np
from jax import lax
from jax.experimental import pallas as pl
from jax.experimental.pallas import tpu as pltpu
from jax.sharding import PartitionSpec as P

N = 128
WINDOWS = 4
HERE = 512
SLABS = 64
ATOMS = SLABS * HERE
high = lax.Precision.HIGH
gauss_width = 2.0


def blocks(real, imaginary):
    return np.block([[real, -imaginary], [imaginary, real]])


def tables():
    k = np.arange(N)
    angle = 2.0 * np.pi * ((k[:, None] * k[None, :]) % N) / N
    cosine, sine = np.cos(angle), np.sin(angle)
    forward = blocks(cosine, -sine)
    inverse = blocks(cosine, sine)
    order = np.arange(2 * N).reshape(2, N // 4, 4).transpose(1, 0, 2).ravel()
    return tuple(
        np.ascontiguousarray(m, dtype=np.float32)
        for m in (
            forward.T,
            forward[order],
            forward,
            inverse,
            inverse[:, order],
            inverse.T,
        )
    )


Y_FORWARD, X_FORWARD, Z_FORWARD, Z_INVERSE, X_INVERSE, Y_INVERSE = tables()


def dot(a, b):
    return jnp.dot(a, b, precision=high, preferred_element_type=jnp.float32)


def weights_of(u):
    v = 1.0 - u
    return (
        v * v * v * (1.0 / 6.0),
        (0.5 * u - 1.0) * u * u + (2.0 / 3.0),
        (0.5 * v - 1.0) * v * v + (2.0 / 3.0),
        u * u * u * (1.0 / 6.0),
    )


def slopes_of(u):
    v = 1.0 - u
    return (-0.5 * v * v, (1.5 * u - 2.0) * u, (2.0 - 1.5 * v) * v, 0.5 * u * u)


def pack_kernel(slab_ref, lambda_ref, a_ref, b_ref, flag_ref, index_ref, weight_ref, out_ref):
    flags = flag_ref[...].astype(jnp.float32)
    steps = flags * (b_ref[...] - a_ref[...])
    first = slab_ref[0] * 2
    out_ref[0] = index_ref[0].astype(jnp.float32)
    out_ref[1] = index_ref[1].astype(jnp.float32)
    out_ref[2] = (index_ref[2] - first).astype(jnp.float32)
    for axis in range(3):
        out_ref[3 + axis] = weight_ref[axis, 2] + 2.0 * weight_ref[axis, 3] - weight_ref[axis, 0]
    row = lax.broadcasted_iota(jnp.int32, (WINDOWS, HERE), 0)
    scale = jnp.zeros((WINDOWS, HERE), jnp.float32)
    for w in range(WINDOWS):
        scale = jnp.where(row == w, lambda_ref[w], scale)
    out_ref[6] = a_ref[...] + scale * steps
    out_ref[7] = steps


def cells(first):
    found = []
    for offset in range(4):
        cell = first + float(offset)
        found.append(jnp.where(cell >= float(N), cell - float(N), cell))
    return found


def spread_table(grid, targets, values):
    out = jnp.zeros(grid.shape, jnp.float32)
    for target, value in zip(targets, values):
        out = jnp.where(grid == target, value, out)
    return out


def plane_parts(source, plane, parts):
    low = plane < 0.5
    if source == 0:
        return jnp.where(low, parts[0], 0.0), jnp.where(low, parts[1], parts[0])
    if source == 1:
        return jnp.where(low, parts[2], parts[1]), jnp.where(low, parts[3], parts[2])
    return jnp.where(low, 0.0, parts[3]), None


def spread_kernel(own_ref, below_ref, far_ref, y_ref, x_ref, out_ref):
    grid = lax.broadcasted_iota(jnp.int32, (N, HERE), 0).astype(jnp.float32)
    planes = []
    for w in range(WINDOWS):
        total = [jnp.zeros((N, N), jnp.float32) for _ in range(2)]
        for source, ref in enumerate((own_ref, below_ref, far_ref)):
            row = lambda r: ref[r, w : w + 1, :]
            charge = row(6)
            depth = plane_parts(source, row(2), weights_of(row(5)))
            along_x = spread_table(grid, cells(row(0)), weights_of(row(3)))
            along_y = spread_table(grid, cells(row(1)), weights_of(row(4)))
            for p in range(2):
                if depth[p] is None:
                    continue
                total[p] = total[p] + lax.dot_general(
                    along_x,
                    along_y * (charge * depth[p]),
                    (((1,), (1,)), ((), ())),
                    precision=high,
                    preferred_element_type=jnp.float32,
                )
        planes.append(total)
    for c in range(2):
        for p in range(2):
            pair = jnp.concatenate([planes[2 * c][p], planes[2 * c + 1][p]], axis=1)
            rows = dot(pair, y_ref[...])
            column = dot(x_ref[...], jnp.concatenate([rows[:, :N], rows[:, N:]], axis=0))
            out_ref[c, :, p] = column.reshape(N // 4, 8, N)


def frequency(counter):
    return jnp.where(counter >= N // 2, counter - N, counter).astype(jnp.float32) / N


def column_kernel(slab_ref, in_ref, forward_ref, inverse_ref, out_ref):
    first = lax.rem(slab_ref[0], 32) * 4
    shape = (N, N)
    freq_z = frequency(lax.broadcasted_iota(jnp.int32, shape, 0))
    freq_y = frequency(lax.broadcasted_iota(jnp.int32, shape, 1))
    flat = freq_z * freq_z + freq_y * freq_y
    for j in range(4):
        freq_x = frequency(jnp.full(shape, first + j, jnp.int32))
        squared = flat + freq_x * freq_x
        positive = squared > 0
        safe = jnp.where(positive, squared, 1.0)
        influence = jnp.where(
            positive, jnp.exp(-gauss_width * squared) / (math.pi * N * N * N * safe), 0.0
        )
        both = jnp.concatenate(
            [in_ref[pl.ds(j, N, stride=8), :], in_ref[pl.ds(4 + j, N, stride=8), :]], axis=0
        )
        depth = dot(forward_ref[...], both)
        depth = depth * jnp.concatenate([influence, influence], axis=0)
        back = dot(inverse_ref[...], depth)
        out_ref[pl.ds(j, N, stride=8), :] = back[:N]
        out_ref[pl.ds(4 + j, N, stride=8), :] = back[N:]


def sample_kernel(
    in_ref, own_ref, below_ref, far_ref, x_ref, y_ref, own_out, below_out, far_out, sum_out
):
    grid = lax.broadcasted_iota(jnp.int32, (N, HERE), 0).astype(jnp.float32)
    planes = [[None, None] for _ in range(WINDOWS)]
    for c in range(2):
        for p in range(2):
            column = dot(x_ref[...], in_ref[c, :, p].reshape(2 * N, N))
            pair = dot(jnp.concatenate([column[:N], column[N:]], axis=1), y_ref[...])
            planes[2 * c][p] = pair[:, :N]
            planes[2 * c + 1][p] = pair[:, N:]
    lane = lax.broadcasted_iota(jnp.int32, (SLABS, N), 1)
    sums = jnp.zeros((SLABS, N), jnp.float32)
    for w in range(WINDOWS):
        energy = jnp.zeros((1, HERE), jnp.float32)
        slope = jnp.zeros((1, HERE), jnp.float32)
        for source, (ref, out_ref) in enumerate(
            ((own_ref, own_out), (below_ref, below_out), (far_ref, far_out))
        ):
            row = lambda r: ref[r, w : w + 1, :]
            charge = row(6)
            depth = plane_parts(source, row(2), weights_of(row(5)))
            steep = plane_parts(source, row(2), slopes_of(row(5)))
            at_x, at_y = cells(row(0)), cells(row(1))
            along_x = spread_table(grid, at_x, weights_of(row(3)))
            steep_x = spread_table(grid, at_x, slopes_of(row(3)))
            along_y = spread_table(grid, at_y, weights_of(row(4)))
            steep_y = spread_table(grid, at_y, slopes_of(row(4)))
            plain = over_z = over_y = None
            for p in range(2):
                if depth[p] is None:
                    continue
                level = dot(planes[w][p], along_y)
                level_y = dot(planes[w][p], steep_y)
                parts = (level * depth[p], level * steep[p], level_y * depth[p])
                if plain is None:
                    plain, over_z, over_y = parts
                else:
                    plain, over_z, over_y = plain + parts[0], over_z + parts[1], over_y + parts[2]
            potential = jnp.sum(along_x * plain, axis=0, keepdims=True)
            out_ref[0, w : w + 1, :] = -charge * jnp.sum(steep_x * plain, axis=0, keepdims=True)
            out_ref[1, w : w + 1, :] = -charge * jnp.sum(along_x * over_y, axis=0, keepdims=True)
            out_ref[2, w : w + 1, :] = -charge * jnp.sum(along_x * over_z, axis=0, keepdims=True)
            energy = energy + charge * potential
            slope = slope + row(7) * potential
        sums = jnp.where(lane == w, jnp.sum(energy, axis=1, keepdims=True), sums)
        sums = jnp.where(lane == WINDOWS + w, jnp.sum(slope, axis=1, keepdims=True), sums)
    sum_out[...] = sums


in_vmem = pl.BlockSpec(memory_space=pltpu.VMEM)
in_smem = pl.BlockSpec(memory_space=pltpu.SMEM)


def f32(*shape):
    return jax.ShapeDtypeStruct(shape, jnp.float32)


def passed_along(value, steps):
    pairs = [(source, (source + steps) % SLABS) for source in range(SLABS)]
    return lax.ppermute(value, "slab", pairs)


def body(lambdas, charge_a, charge_b, perturbed, grid_index, spline_weights, spline_slopes):
    slab = lax.axis_index("slab").reshape(1)
    own = pl.pallas_call(
        pack_kernel,
        out_shape=f32(8, WINDOWS, HERE),
        in_specs=[in_smem, in_smem] + [in_vmem] * 5,
        out_specs=in_vmem,
        name="pack",
    )(slab, lambdas, charge_a, charge_b, perturbed, grid_index, spline_weights)
    below = passed_along(own, 1)
    far = passed_along(own, 2)
    spectrum = pl.pallas_call(
        spread_kernel,
        out_shape=f32(2, N // 4, 2, 8, N),
        in_specs=[in_vmem] * 5,
        out_specs=in_vmem,
        name="spread",
    )(own, below, far, Y_FORWARD, X_FORWARD)
    columns = lax.all_to_all(spectrum.reshape(SLABS, 16, N), "slab", 0, 0, tiled=True)
    columns = pl.pallas_call(
        column_kernel,
        out_shape=f32(8 * N, N),
        in_specs=[in_smem] + [in_vmem] * 3,
        out_specs=in_vmem,
        name="columns",
    )(slab, columns.reshape(8 * N, N), Z_FORWARD, Z_INVERSE)
    levels = lax.all_to_all(columns.reshape(SLABS, 16, N), "slab", 0, 0, tiled=True)
    part = f32(3, WINDOWS, HERE)
    mine, for_below, for_far, sums = pl.pallas_call(
        sample_kernel,
        out_shape=(part, part, part, f32(SLABS, N)),
        in_specs=[in_vmem] * 6,
        out_specs=(in_vmem,) * 4,
        name="sample",
    )(levels.reshape(2, N // 4, 2, 8, N), own, below, far, X_INVERSE, Y_INVERSE)
    from_above = passed_along(for_below, -1)
    from_far = passed_along(for_far, -2)
    sums = lax.all_to_all(sums.reshape(SLABS, 1, N), "slab", 0, 0, tiled=True)
    sums = jnp.sum(sums, axis=(0, 1))
    return (
        mine + from_above + from_far,
        sums[:WINDOWS] * (0.5 / ATOMS),
        sums[WINDOWS : 2 * WINDOWS] * (1.0 / ATOMS),
    )


def solution(mesh):
    return jax.shard_map(
        body,
        mesh=mesh,
        in_specs=(
            P("win"),
            P("win", "slab"),
            P("win", "slab"),
            P("win", "slab"),
            P(None, "win", "slab"),
            P(None, None, "win", "slab"),
            P(None, None, "win", "slab"),
        ),
        out_specs=(P(None, "win", "slab"), P("win"), P("win")),
        check_vma=False,
    )
```

```python
import math

import jax
import jax.numpy as jnp
import numpy as np
from jax import lax
from jax.experimental import pallas as pl
from jax.experimental.pallas import tpu as pltpu
from jax.sharding import PartitionSpec as P

N = 128
LANES = 128
WINDOWS = 4
HERE = 512
SLABS = 64
ATOMS = SLABS * HERE
gauss_width = 2.0


def blocks(real, imaginary):
    return np.block([[real, -imaginary], [imaginary, real]])


def tables():
    k = np.arange(N)
    angle = 2.0 * np.pi * ((k[:, None] * k[None, :]) % N) / N
    cosine, sine = np.cos(angle), np.sin(angle)
    forward = blocks(cosine, -sine)
    inverse = blocks(cosine, sine)
    order = np.arange(2 * N).reshape(2, N // 4, 4).transpose(1, 0, 2).ravel()
    return tuple(
        np.ascontiguousarray(m, dtype=np.float32)
        for m in (
            forward.T,
            forward[order],
            forward,
            inverse,
            inverse[:, order],
            inverse.T,
        )
    )


def halves(x):
    top = x.astype(jnp.bfloat16)
    return top, (x - top.astype(jnp.float32)).astype(jnp.bfloat16)


def table_halves(table):
    top = table.astype(jnp.bfloat16)
    return np.stack([top, (table - top.astype(np.float32)).astype(jnp.bfloat16)])


Y_FORWARD, X_FORWARD, Z_FORWARD, Z_INVERSE, X_INVERSE, Y_INVERSE = map(table_halves, tables())


def dot(a, b, contract=(1, 0)):
    dims = (((contract[0],), (contract[1],)), ((), ()))
    return lax.dot_general(a, b, dims, preferred_element_type=jnp.float32)


def table_times(table_ref, x):
    top, rest = halves(x)
    return dot(table_ref[0], top) + dot(table_ref[1], top) + dot(table_ref[0], rest)


def times_table(x, table_ref):
    top, rest = halves(x)
    return dot(top, table_ref[0]) + dot(rest, table_ref[0]) + dot(top, table_ref[1])


def weights_of(u):
    v = 1.0 - u
    return (
        v * v * v * (1.0 / 6.0),
        (0.5 * u - 1.0) * u * u + (2.0 / 3.0),
        (0.5 * v - 1.0) * v * v + (2.0 / 3.0),
        u * u * u * (1.0 / 6.0),
    )


def slopes_of(u):
    v = 1.0 - u
    return (-0.5 * v * v, (1.5 * u - 2.0) * u, (2.0 - 1.5 * v) * v, 0.5 * u * u)


def pack_kernel(slab_ref, *refs):
    sources, out_ref, landed, sem = refs[:6], refs[6], refs[7:13], refs[13]
    copies = [
        pltpu.make_async_copy(source, target, sem.at[i])
        for i, (source, target) in enumerate(zip(sources, landed))
    ]
    for copy in copies:
        copy.start()
    for copy in copies:
        copy.wait()
    lambda_ref, a_ref, b_ref, flag_ref, index_ref, weight_ref = landed
    flags = flag_ref[...].astype(jnp.float32)
    steps = flags * (b_ref[...] - a_ref[...])
    first = slab_ref[0] * 2
    out_ref[0] = index_ref[0].astype(jnp.float32)
    out_ref[1] = index_ref[1].astype(jnp.float32)
    out_ref[2] = (index_ref[2] - first).astype(jnp.float32)
    for axis in range(3):
        out_ref[3 + axis] = weight_ref[axis, 2] + 2.0 * weight_ref[axis, 3] - weight_ref[axis, 0]
    row = lax.broadcasted_iota(jnp.int32, (WINDOWS, HERE), 0)
    scale = jnp.zeros((WINDOWS, HERE), jnp.float32)
    for w in range(WINDOWS):
        scale = jnp.where(row == w, lambda_ref[w], scale)
    out_ref[6] = a_ref[...] + scale * steps
    out_ref[7] = steps


def places(first, height):
    block = jnp.floor(first * (1.0 / height))
    after = jnp.where(block == float(N // height - 1), 0.0, block + 1.0)
    return block, after, first - height * block


def row_halves(value):
    top = value.astype(jnp.bfloat16).astype(jnp.float32)
    return top, value - top


def wide(row):
    return jnp.broadcast_to(row, (16, LANES)).astype(jnp.bfloat16)


def tall(row):
    return jnp.broadcast_to(row, (8, LANES))


def rows_of(height):
    return lax.broadcasted_iota(jnp.int32, (height, LANES), 0).astype(jnp.float32)


def stencil_tiles(rows, height, start, columns):
    zero = jnp.zeros_like(rows)
    here = [rows == start + jnp.asarray(k, rows.dtype) for k in range(4)]
    past = [rows + jnp.asarray(height, rows.dtype) == start + jnp.asarray(k, rows.dtype) for k in range(1, 4)]
    tiles = []
    for values in columns:
        first = second = zero
        for k in range(4):
            first = jnp.where(here[k], values[k], first)
        for k in range(1, 4):
            second = jnp.where(past[k - 1], values[k], second)
        tiles.append((first, second))
    return tiles


def table_columns(block, after, tiles):
    columns = [[] for _ in tiles]
    zero = jnp.zeros_like(tiles[0][0])
    for b in range(N // 16):
        at, next_at = block == jnp.asarray(b, block.dtype), after == jnp.asarray(b, block.dtype)
        for column, (first, second) in zip(columns, tiles):
            column.append(jnp.where(at, first, jnp.where(next_at, second, zero)))
    return [jnp.concatenate(column, axis=0) for column in columns]


def plane_parts(source, plane, parts):
    low = plane < 0.5
    if source == 0:
        return jnp.where(low, parts[0], 0.0), jnp.where(low, parts[1], parts[0])
    if source == 1:
        return jnp.where(low, parts[2], parts[1]), jnp.where(low, parts[3], parts[2])
    return jnp.where(low, 0.0, parts[3]), None


def spread_rows(source, ref, keep):
    block, after, row = places(ref[0], 16)
    keep[0], keep[1], keep[2] = block, after, row
    block, after, row = places(ref[1], 16)
    keep[3], keep[4], keep[5] = block, after, row
    for k, value in enumerate(weights_of(ref[3])):
        keep[6 + k], keep[10 + k] = row_halves(value)
    along_y = weights_of(ref[4])
    for p, depth in enumerate(plane_parts(source, ref[2], weights_of(ref[5]))):
        if depth is not None:
            for k in range(4):
                top, rest = row_halves(along_y[k] * (ref[6] * depth))
                keep[14 + 8 * p + k], keep[18 + 8 * p + k] = top, rest


def spread_planes(sources, keep):
    for slot, (source, ref) in enumerate(sources):
        spread_rows(source, ref, keep.at[slot])
    rows16 = rows_of(16).astype(jnp.bfloat16)
    blank = jnp.zeros((N, LANES), jnp.bfloat16)
    planes = []
    for w in range(WINDOWS):
        left, right_top, right_rest = [], [], []
        for slot, (source, ref) in enumerate(sources):
            for chunk in range(HERE // LANES):
                lanes = slice(chunk * LANES, (chunk + 1) * LANES)
                row = lambda r: wide(keep[slot, r, w : w + 1, lanes])
                four = lambda r: [row(r + k) for k in range(4)]
                tiles = stencil_tiles(rows16, 16, row(2), [four(6), four(10)])
                left.append(jnp.concatenate(table_columns(row(0), row(1), tiles), axis=0))
                count = 1 if source == 2 else 2
                tiles = stencil_tiles(
                    rows16, 16, row(5), [four(14 + 4 * i) for i in range(2 * count)]
                )
                found = table_columns(row(3), row(4), tiles)
                if count == 1:
                    found = found + [blank, blank]
                right_top.append(jnp.concatenate([found[0], found[2]], axis=0))
                right_rest.append(jnp.concatenate([found[1], found[3]], axis=0))
        left = jnp.concatenate(left, axis=1)
        both = dot(left, jnp.concatenate(right_top, axis=1), (1, 1))
        rest = dot(left[:N], jnp.concatenate(right_rest, axis=1), (1, 1))
        planes.append(both[:N] + both[N:] + rest)
    return planes


def own_spread_kernel(own_ref, out_ref, keep):
    for w, planes in enumerate(spread_planes(((0, own_ref),), keep)):
        out_ref[w] = planes


def spread_kernel(own_ref, below_ref, far_ref, y_hbm, x_hbm, out_ref, keep, y_ref, x_ref, sem):
    copies = [
        pltpu.make_async_copy(y_hbm, y_ref, sem.at[0]),
        pltpu.make_async_copy(x_hbm, x_ref, sem.at[1]),
    ]
    for copy in copies:
        copy.start()
    planes = spread_planes(((1, below_ref), (2, far_ref)), keep)
    planes = [own_ref[w] + planes[w] for w in range(WINDOWS)]
    for copy in copies:
        copy.wait()
    stacked = jnp.concatenate(
        [
            jnp.concatenate([planes[2 * c][:, cut], planes[2 * c + 1][:, cut]], axis=1)
            for c in range(2)
            for cut in (slice(0, N), slice(N, 2 * N))
        ],
        axis=0,
    )
    turned = times_table(stacked, y_ref)
    upright = jnp.concatenate(
        [
            jnp.concatenate([turned[b * N : b * N + N, :N], turned[b * N : b * N + N, N:]], axis=0)
            for b in range(4)
        ],
        axis=1,
    )
    columns = table_times(x_ref, upright)
    for b in range(4):
        out_ref[b // 2, :, b % 2] = columns[:, b * N : b * N + N].reshape(N // 4, 8, N)


def frequency(counter):
    return jnp.where(counter >= N // 2, counter - N, counter).astype(jnp.float32) / N


def influence_kernel(slab_ref, out_ref):
    first = lax.rem(slab_ref[0], SLABS // 2) * 4
    shape = (N, N)
    freq_z = frequency(lax.broadcasted_iota(jnp.int32, shape, 0))
    freq_y = frequency(lax.broadcasted_iota(jnp.int32, shape, 1))
    flat = freq_z * freq_z + freq_y * freq_y
    for j in range(4):
        freq_x = frequency(jnp.full(shape, first + j, jnp.int32))
        squared = flat + freq_x * freq_x
        positive = squared > 0
        safe = jnp.where(positive, squared, 1.0)
        out_ref[:, j * N : j * N + N] = jnp.where(
            positive, jnp.exp(-gauss_width * squared) / (math.pi * N * N * N * safe), 0.0
        )


def column_kernel(in_ref, influence_ref, forward_ref, inverse_ref, out_ref):
    part = lambda r: in_ref[pl.ds(r, N, stride=8), :]
    columns = jnp.concatenate(
        [jnp.concatenate([part(j), part(4 + j)], axis=0) for j in range(4)], axis=1
    )
    depth = table_times(forward_ref, columns)
    influence = influence_ref[...]
    depth = jnp.concatenate([depth[:N] * influence, depth[N:] * influence], axis=0)
    back = table_times(inverse_ref, depth)
    for j in range(4):
        out_ref[pl.ds(j, N, stride=8), :] = back[:N, j * N : j * N + N]
        out_ref[pl.ds(4 + j, N, stride=8), :] = back[N:, j * N : j * N + N]


def sample_rows(source, ref, keep):
    block, after, row = places(ref[1], 16)
    keep[0], keep[1], keep[2] = block, after, row
    for k, value in enumerate(weights_of(ref[4])):
        keep[3 + k], keep[7 + k] = row_halves(value)
    for k, value in enumerate(slopes_of(ref[4])):
        keep[11 + k], keep[15 + k] = row_halves(value)
    block, after, row = places(ref[0], 8)
    keep[19], keep[20], keep[21] = block, after, row
    for k, (value, slope) in enumerate(zip(weights_of(ref[3]), slopes_of(ref[3]))):
        keep[22 + k], keep[26 + k] = value, slope
    depth = plane_parts(source, ref[2], weights_of(ref[5]))
    steep = plane_parts(source, ref[2], slopes_of(ref[5]))
    for p in range(2):
        if depth[p] is not None:
            keep[30 + p], keep[32 + p] = depth[p], steep[p]


def sample_kernel(
    in_ref, own_ref, below_ref, far_ref, x_ref, y_ref, own_out, below_out, far_out, sum_out, keep, sums
):
    sources = ((0, own_ref, own_out), (1, below_ref, below_out), (2, far_ref, far_out))
    columns = jnp.concatenate(
        [in_ref[b // 2, :, b % 2].reshape(2 * N, N) for b in range(4)], axis=1
    )
    upright = table_times(x_ref, columns)
    flat = jnp.concatenate(
        [
            jnp.concatenate([upright[:N, b * N : b * N + N], upright[N:, b * N : b * N + N]], axis=1)
            for b in range(4)
        ],
        axis=0,
    )
    pairs = times_table(flat, y_ref)
    for source, ref, _ in sources:
        sample_rows(source, ref, keep.at[source])
    rows16 = rows_of(16).astype(jnp.bfloat16)
    rows8 = rows_of(8)
    for w in range(WINDOWS):
        side = slice((w % 2) * N, (w % 2) * N + N)
        start = (w // 2) * 2 * N
        planes = jnp.concatenate(halves(pairs[start : start + 2 * N, side]), axis=1)
        energy = jnp.zeros((1, LANES), jnp.float32)
        slope = jnp.zeros((1, LANES), jnp.float32)
        for source, ref, out_ref in sources:
            tops, rests = [], []
            for chunk in range(HERE // LANES):
                lanes = slice(chunk * LANES, (chunk + 1) * LANES)
                row = lambda r: wide(keep[source, r, w : w + 1, lanes])
                four = lambda r: [row(r + k) for k in range(4)]
                tiles = stencil_tiles(rows16, 16, row(2), [four(3 + 4 * i) for i in range(4)])
                found = table_columns(row(0), row(1), tiles)
                tops.append(jnp.concatenate([found[0], found[2]], axis=1))
                rests.append(jnp.concatenate([found[1], found[3]], axis=1))
            count = 1 if source == 2 else 2
            tops = jnp.concatenate(tops, axis=1)
            rests = jnp.concatenate(rests, axis=1)
            used = planes[: count * N]
            levels = dot(used, jnp.concatenate([tops, tops], axis=0)) + dot(used[:, :N], rests)
            for chunk in range(HERE // LANES):
                lanes = slice(chunk * LANES, (chunk + 1) * LANES)
                row = lambda r: tall(keep[source, r, w : w + 1, lanes])
                four = lambda r: [row(r + k) for k in range(4)]
                block, after = row(19), row(20)
                tiles = stencil_tiles(rows8, 8, row(21), [four(22), four(26)])
                near = [[None] * 2 for _ in range(2 * count)]
                for b in range(N // 8):
                    at, next_at = block == float(b), after == float(b)
                    for q in range(2 * count):
                        p, kind = q // 2, q % 2
                        level = levels[
                            p * N + b * 8 : p * N + b * 8 + 8,
                            (2 * chunk + kind) * LANES : (2 * chunk + kind + 1) * LANES,
                        ]
                        if b == 0:
                            near[q] = [level, level]
                        else:
                            near[q][0] = jnp.where(at, level, near[q][0])
                            near[q][1] = jnp.where(next_at, level, near[q][1])
                total = [jnp.zeros((8, LANES), jnp.float32) for _ in range(4)]
                for half in range(2):
                    along, along_dx = tiles[0][half], tiles[1][half]
                    plain = near[0][half] * row(30)
                    over_z = near[0][half] * row(32)
                    over_y = near[1][half] * row(30)
                    if count == 2:
                        plain = plain + near[2][half] * row(31)
                        over_z = over_z + near[2][half] * row(33)
                        over_y = over_y + near[3][half] * row(31)
                    total[0] = total[0] + along * plain
                    total[1] = total[1] + along_dx * plain
                    total[2] = total[2] + along * over_y
                    total[3] = total[3] + along * over_z
                total = [jnp.sum(t, axis=0, keepdims=True) for t in total]
                charge = ref[6, w : w + 1, lanes]
                for d in range(3):
                    out_ref[d, w : w + 1, lanes] = -charge * total[1 + d]
                energy = energy + charge * total[0]
                slope = slope + ref[7, w : w + 1, lanes] * total[0]
        sums[w : w + 1, :] = energy
        sums[WINDOWS + w : WINDOWS + w + 1, :] = slope
    added = jnp.sum(sums[...], axis=1, keepdims=True)
    shape = (8, LANES)
    here = lax.broadcasted_iota(jnp.int32, shape, 0) == lax.broadcasted_iota(jnp.int32, shape, 1)
    line = jnp.sum(jnp.where(here, added, 0.0), axis=0, keepdims=True)
    sum_out[...] = jnp.broadcast_to(line, (SLABS, LANES))


in_vmem = pl.BlockSpec(memory_space=pltpu.VMEM)
in_smem = pl.BlockSpec(memory_space=pltpu.SMEM)
in_hbm = pl.BlockSpec(memory_space=pltpu.HBM)
table_scratch = pltpu.VMEM((2, 2 * N, 2 * N), jnp.bfloat16)


def f32(*shape):
    return jax.ShapeDtypeStruct(shape, jnp.float32)


def run(kernel, out_shape, in_specs, operands, scratch=(), mib=16):
    several = isinstance(out_shape, tuple)
    return pl.pallas_call(
        kernel,
        out_shape=out_shape,
        in_specs=in_specs,
        out_specs=(in_vmem,) * len(out_shape) if several else in_vmem,
        scratch_shapes=list(scratch),
        compiler_params=pltpu.CompilerParams(vmem_limit_bytes=mib << 20),
        name=kernel.__name__,
    )(*operands)


def passed_along(value, steps):
    pairs = [(source, (source + steps) % SLABS) for source in range(SLABS)]
    return lax.ppermute(value, "slab", pairs)


def body(lambdas, charge_a, charge_b, perturbed, grid_index, spline_weights, spline_slopes):
    slab = lax.axis_index("slab").reshape(1)
    inputs = (lambdas, charge_a, charge_b, perturbed, grid_index, spline_weights)
    own = run(
        pack_kernel,
        f32(8, WINDOWS, HERE),
        [in_smem] + [in_hbm] * 6,
        (slab, *inputs),
        [pltpu.SMEM((WINDOWS,), jnp.float32)]
        + [pltpu.VMEM(a.shape, a.dtype) for a in inputs[1:]]
        + [pltpu.SemaphoreType.DMA((6,))],
        mib=4,
    )
    below = passed_along(own, 1)
    far = passed_along(own, 2)
    kept = lambda count, rows: pltpu.VMEM((count, rows, WINDOWS, HERE), jnp.float32)
    from_own = run(
        own_spread_kernel, f32(WINDOWS, N, 2 * N), [in_vmem], (own,), [kept(1, 30)]
    )
    spectrum = run(
        spread_kernel,
        f32(2, N // 4, 2, 8, N),
        [in_vmem] * 3 + [in_hbm] * 2,
        (from_own, below, far, Y_FORWARD, X_FORWARD),
        [kept(2, 30), table_scratch, table_scratch, pltpu.SemaphoreType.DMA((2,))],
    )
    influence = run(influence_kernel, f32(N, 4 * N), [in_smem], (slab,), mib=4)
    columns = lax.all_to_all(spectrum.reshape(SLABS, 16, N), "slab", 0, 0, tiled=True)
    columns = run(
        column_kernel,
        f32(8 * N, N),
        [in_vmem] * 4,
        (columns.reshape(8 * N, N), influence, Z_FORWARD, Z_INVERSE),
        mib=8,
    )
    levels = lax.all_to_all(columns.reshape(SLABS, 16, N), "slab", 0, 0, tiled=True)
    part = f32(3, WINDOWS, HERE)
    mine, for_below, for_far, sums = run(
        sample_kernel,
        (part, part, part, f32(SLABS, N)),
        [in_vmem] * 6,
        (levels.reshape(2, N // 4, 2, 8, N), own, below, far, X_INVERSE, Y_INVERSE),
        [kept(3, 34), pltpu.VMEM((8, LANES), jnp.float32)],
    )
    from_above = passed_along(for_below, -1)
    from_far = passed_along(for_far, -2)
    sums = lax.all_to_all(sums.reshape(SLABS, 1, N), "slab", 0, 0, tiled=True)
    sums = jnp.sum(sums, axis=(0, 1))
    return (
        mine + from_above + from_far,
        sums[:WINDOWS] * (0.5 / ATOMS),
        sums[WINDOWS : 2 * WINDOWS] * (1.0 / ATOMS),
    )


def solution(mesh):
    return jax.shard_map(
        body,
        mesh=mesh,
        in_specs=(
            P("win"),
            P("win", "slab"),
            P("win", "slab"),
            P("win", "slab"),
            P(None, "win", "slab"),
            P(None, None, "win", "slab"),
            P(None, None, "win", "slab"),
        ),
        out_specs=(P(None, "win", "slab"), P("win"), P("win")),
        check_vma=False,
    )
```

```python
import math

import jax
import jax.numpy as jnp
import numpy as np
from jax import lax
from jax.experimental import pallas as pl
from jax.experimental.pallas import tpu as pltpu
from jax.sharding import PartitionSpec as P

N = 128
LANES = 128
WINDOWS = 4
HERE = 512
SLABS = 64
ATOMS = SLABS * HERE
gauss_width = 2.0


def blocks(real, imaginary):
    return np.block([[real, -imaginary], [imaginary, real]])


def tables():
    k = np.arange(N)
    angle = 2.0 * np.pi * ((k[:, None] * k[None, :]) % N) / N
    cosine, sine = np.cos(angle), np.sin(angle)
    forward = blocks(cosine, -sine)
    inverse = blocks(cosine, sine)
    order = np.arange(2 * N).reshape(2, N // 4, 4).transpose(1, 0, 2).ravel()
    return tuple(
        np.ascontiguousarray(m, dtype=np.float32)
        for m in (
            forward.T,
            forward[order],
            forward,
            inverse,
            inverse[:, order],
            inverse.T,
        )
    )


def halves(x):
    top = x.astype(jnp.bfloat16)
    return top, (x - top.astype(jnp.float32)).astype(jnp.bfloat16)


def table_halves(table):
    top = table.astype(jnp.bfloat16)
    return np.stack([top, (table - top.astype(np.float32)).astype(jnp.bfloat16)])


Y_FORWARD, X_FORWARD, Z_FORWARD, Z_INVERSE, X_INVERSE, Y_INVERSE = map(table_halves, tables())


def dot(a, b, contract=(1, 0)):
    dims = (((contract[0],), (contract[1],)), ((), ()))
    return lax.dot_general(a, b, dims, preferred_element_type=jnp.float32)


def table_times(table_ref, x):
    top, rest = halves(x)
    return dot(table_ref[0], top) + dot(table_ref[1], top) + dot(table_ref[0], rest)


def times_table(x, table_ref):
    top, rest = halves(x)
    return dot(top, table_ref[0]) + dot(rest, table_ref[0]) + dot(top, table_ref[1])


def weights_of(u):
    v = 1.0 - u
    return (
        v * v * v * (1.0 / 6.0),
        (0.5 * u - 1.0) * u * u + (2.0 / 3.0),
        (0.5 * v - 1.0) * v * v + (2.0 / 3.0),
        u * u * u * (1.0 / 6.0),
    )


def slopes_of(u):
    v = 1.0 - u
    return (-0.5 * v * v, (1.5 * u - 2.0) * u, (2.0 - 1.5 * v) * v, 0.5 * u * u)


def pack_kernel(slab_ref, *refs):
    sources, out_ref, landed, sem = refs[:6], refs[6], refs[7:13], refs[13]
    copies = [
        pltpu.make_async_copy(source, target, sem.at[i])
        for i, (source, target) in enumerate(zip(sources, landed))
    ]
    for copy in copies:
        copy.start()
    for copy in copies:
        copy.wait()
    lambda_ref, a_ref, b_ref, flag_ref, index_ref, weight_ref = landed
    flags = flag_ref[...].astype(jnp.float32)
    steps = flags * (b_ref[...] - a_ref[...])
    first = slab_ref[0] * 2
    out_ref[0] = index_ref[0].astype(jnp.float32)
    out_ref[1] = index_ref[1].astype(jnp.float32)
    out_ref[2] = (index_ref[2] - first).astype(jnp.float32)
    for axis in range(3):
        out_ref[3 + axis] = weight_ref[axis, 2] + 2.0 * weight_ref[axis, 3] - weight_ref[axis, 0]
    row = lax.broadcasted_iota(jnp.int32, (WINDOWS, HERE), 0)
    scale = jnp.zeros((WINDOWS, HERE), jnp.float32)
    for w in range(WINDOWS):
        scale = jnp.where(row == w, lambda_ref[w], scale)
    out_ref[6] = a_ref[...] + scale * steps
    out_ref[7] = steps


def places(first, height):
    block = jnp.floor(first * (1.0 / height))
    after = jnp.where(block == float(N // height - 1), 0.0, block + 1.0)
    return block, after, first - height * block


def row_halves(value):
    top = value.astype(jnp.bfloat16).astype(jnp.float32)
    return top, value - top


def wide(row):
    return jnp.broadcast_to(row, (16, LANES)).astype(jnp.bfloat16)


def tall(row):
    return jnp.broadcast_to(row, (8, LANES))


def rows_of(height):
    return lax.broadcasted_iota(jnp.int32, (height, LANES), 0).astype(jnp.float32)


def stencil_tiles(rows, height, start, columns):
    zero = jnp.zeros_like(rows)
    here = [rows == start + jnp.asarray(k, rows.dtype) for k in range(4)]
    past = [rows + jnp.asarray(height, rows.dtype) == start + jnp.asarray(k, rows.dtype) for k in range(1, 4)]
    tiles = []
    for values in columns:
        first = second = zero
        for k in range(4):
            first = jnp.where(here[k], values[k], first)
        for k in range(1, 4):
            second = jnp.where(past[k - 1], values[k], second)
        tiles.append((first, second))
    return tiles


def table_columns(block, after, tiles):
    columns = [[] for _ in tiles]
    zero = jnp.zeros_like(tiles[0][0])
    for b in range(N // 16):
        at, next_at = block == jnp.asarray(b, block.dtype), after == jnp.asarray(b, block.dtype)
        for column, (first, second) in zip(columns, tiles):
            column.append(jnp.where(at, first, jnp.where(next_at, second, zero)))
    return [jnp.concatenate(column, axis=0) for column in columns]


def plane_parts(source, plane, parts):
    low = plane < 0.5
    if source == 0:
        return jnp.where(low, parts[0], 0.0), jnp.where(low, parts[1], parts[0])
    if source == 1:
        return jnp.where(low, parts[2], parts[1]), jnp.where(low, parts[3], parts[2])
    return jnp.where(low, 0.0, parts[3]), None


def spread_rows(source, ref, keep):
    block, after, row = places(ref[0], 16)
    keep[0], keep[1], keep[2] = block, after, row
    block, after, row = places(ref[1], 16)
    keep[3], keep[4], keep[5] = block, after, row
    for k, value in enumerate(weights_of(ref[3])):
        keep[6 + k], keep[10 + k] = row_halves(value)
    along_y = weights_of(ref[4])
    for p, depth in enumerate(plane_parts(source, ref[2], weights_of(ref[5]))):
        if depth is not None:
            for k in range(4):
                top, rest = row_halves(along_y[k] * (ref[6] * depth))
                keep[14 + 8 * p + k], keep[18 + 8 * p + k] = top, rest


def spread_planes(sources, keep):
    for slot, (source, ref) in enumerate(sources):
        spread_rows(source, ref, keep.at[slot])
    rows16 = rows_of(16).astype(jnp.bfloat16)
    blank = jnp.zeros((N, LANES), jnp.bfloat16)
    planes = []
    for w in range(WINDOWS):
        left, right_top, right_rest = [], [], []
        for slot, (source, ref) in enumerate(sources):
            for chunk in range(HERE // LANES):
                lanes = slice(chunk * LANES, (chunk + 1) * LANES)
                row = lambda r: wide(keep[slot, r, w : w + 1, lanes])
                four = lambda r: [row(r + k) for k in range(4)]
                tiles = stencil_tiles(rows16, 16, row(2), [four(6), four(10)])
                left.append(jnp.concatenate(table_columns(row(0), row(1), tiles), axis=0))
                count = 1 if source == 2 else 2
                tiles = stencil_tiles(
                    rows16, 16, row(5), [four(14 + 4 * i) for i in range(2 * count)]
                )
                found = table_columns(row(3), row(4), tiles)
                if count == 1:
                    found = found + [blank, blank]
                right_top.append(jnp.concatenate([found[0], found[2]], axis=0))
                right_rest.append(jnp.concatenate([found[1], found[3]], axis=0))
        left = jnp.concatenate(left, axis=1)
        both = dot(left, jnp.concatenate(right_top, axis=1), (1, 1))
        rest = dot(left[:N], jnp.concatenate(right_rest, axis=1), (1, 1))
        planes.append(both[:N] + both[N:] + rest)
    return planes


def own_spread_kernel(slab_ref, own_ref, out_ref, influence_ref, keep):
    fill_influence(slab_ref, influence_ref)
    for w, planes in enumerate(spread_planes(((0, own_ref),), keep)):
        out_ref[w] = planes


def spread_kernel(own_ref, below_ref, far_ref, y_hbm, x_hbm, out_ref, keep, y_ref, x_ref, sem):
    copies = [
        pltpu.make_async_copy(y_hbm, y_ref, sem.at[0]),
        pltpu.make_async_copy(x_hbm, x_ref, sem.at[1]),
    ]
    for copy in copies:
        copy.start()
    planes = spread_planes(((1, below_ref), (2, far_ref)), keep)
    planes = [own_ref[w] + planes[w] for w in range(WINDOWS)]
    for copy in copies:
        copy.wait()
    stacked = jnp.concatenate(
        [
            jnp.concatenate([planes[2 * c][:, cut], planes[2 * c + 1][:, cut]], axis=1)
            for c in range(2)
            for cut in (slice(0, N), slice(N, 2 * N))
        ],
        axis=0,
    )
    turned = times_table(stacked, y_ref)
    upright = jnp.concatenate(
        [
            jnp.concatenate([turned[b * N : b * N + N, :N], turned[b * N : b * N + N, N:]], axis=0)
            for b in range(4)
        ],
        axis=1,
    )
    columns = table_times(x_ref, upright)
    for b in range(4):
        out_ref[b // 2, :, b % 2] = columns[:, b * N : b * N + N].reshape(N // 4, 8, N)


def frequency(counter):
    return jnp.where(counter >= N // 2, counter - N, counter).astype(jnp.float32) / N


def fill_influence(slab_ref, out_ref):
    first = lax.rem(slab_ref[0], SLABS // 2) * 4
    shape = (N, N)
    freq_z = frequency(lax.broadcasted_iota(jnp.int32, shape, 0))
    freq_y = frequency(lax.broadcasted_iota(jnp.int32, shape, 1))
    flat = freq_z * freq_z + freq_y * freq_y
    for j in range(4):
        freq_x = frequency(jnp.full(shape, first + j, jnp.int32))
        squared = flat + freq_x * freq_x
        positive = squared > 0
        safe = jnp.where(positive, squared, 1.0)
        out_ref[:, j * N : j * N + N] = jnp.where(
            positive, jnp.exp(-gauss_width * squared) / (math.pi * N * N * N * safe), 0.0
        )


def column_kernel(in_ref, influence_ref, forward_ref, inverse_ref, out_ref):
    part = lambda r: in_ref[pl.ds(r, N, stride=8), :]
    columns = jnp.concatenate(
        [jnp.concatenate([part(j), part(4 + j)], axis=0) for j in range(4)], axis=1
    )
    depth = table_times(forward_ref, columns)
    influence = influence_ref[...]
    depth = jnp.concatenate([depth[:N] * influence, depth[N:] * influence], axis=0)
    back = table_times(inverse_ref, depth)
    for j in range(4):
        out_ref[pl.ds(j, N, stride=8), :] = back[:N, j * N : j * N + N]
        out_ref[pl.ds(4 + j, N, stride=8), :] = back[N:, j * N : j * N + N]


def sample_rows(source, ref, keep):
    block, after, row = places(ref[1], 16)
    keep[0], keep[1], keep[2] = block, after, row
    for k, value in enumerate(weights_of(ref[4])):
        keep[3 + k], keep[7 + k] = row_halves(value)
    for k, value in enumerate(slopes_of(ref[4])):
        keep[11 + k], keep[15 + k] = row_halves(value)
    block, after, row = places(ref[0], 8)
    keep[19], keep[20], keep[21] = block, after, row
    for k, (value, slope) in enumerate(zip(weights_of(ref[3]), slopes_of(ref[3]))):
        keep[22 + k], keep[26 + k] = value, slope
    depth = plane_parts(source, ref[2], weights_of(ref[5]))
    steep = plane_parts(source, ref[2], slopes_of(ref[5]))
    for p in range(2):
        if depth[p] is not None:
            keep[30 + p], keep[32 + p] = depth[p], steep[p]


def sample_kernel(
    in_ref, own_ref, below_ref, far_ref, x_ref, y_ref, own_out, below_out, far_out, sum_out, keep, sums
):
    sources = ((0, own_ref, own_out), (1, below_ref, below_out), (2, far_ref, far_out))
    columns = jnp.concatenate(
        [in_ref[b // 2, :, b % 2].reshape(2 * N, N) for b in range(4)], axis=1
    )
    upright = table_times(x_ref, columns)
    flat = jnp.concatenate(
        [
            jnp.concatenate([upright[:N, b * N : b * N + N], upright[N:, b * N : b * N + N]], axis=1)
            for b in range(4)
        ],
        axis=0,
    )
    pairs = times_table(flat, y_ref)
    for source, ref, _ in sources:
        sample_rows(source, ref, keep.at[source])
    rows16 = rows_of(16).astype(jnp.bfloat16)
    rows8 = rows_of(8)
    for w in range(WINDOWS):
        side = slice((w % 2) * N, (w % 2) * N + N)
        start = (w // 2) * 2 * N
        planes = jnp.concatenate(halves(pairs[start : start + 2 * N, side]), axis=1)
        energy = jnp.zeros((1, LANES), jnp.float32)
        slope = jnp.zeros((1, LANES), jnp.float32)
        for source, ref, out_ref in sources:
            tops, rests = [], []
            for chunk in range(HERE // LANES):
                lanes = slice(chunk * LANES, (chunk + 1) * LANES)
                row = lambda r: wide(keep[source, r, w : w + 1, lanes])
                four = lambda r: [row(r + k) for k in range(4)]
                tiles = stencil_tiles(rows16, 16, row(2), [four(3 + 4 * i) for i in range(4)])
                found = table_columns(row(0), row(1), tiles)
                tops.append(jnp.concatenate([found[0], found[2]], axis=1))
                rests.append(jnp.concatenate([found[1], found[3]], axis=1))
            count = 1 if source == 2 else 2
            tops = jnp.concatenate(tops, axis=1)
            rests = jnp.concatenate(rests, axis=1)
            used = planes[: count * N]
            levels = dot(used, jnp.concatenate([tops, tops], axis=0)) + dot(used[:, :N], rests)
            for chunk in range(HERE // LANES):
                lanes = slice(chunk * LANES, (chunk + 1) * LANES)
                row = lambda r: tall(keep[source, r, w : w + 1, lanes])
                four = lambda r: [row(r + k) for k in range(4)]
                block, after = row(19), row(20)
                tiles = stencil_tiles(rows8, 8, row(21), [four(22), four(26)])
                near = [[None] * 2 for _ in range(2 * count)]
                for b in range(N // 8):
                    at, next_at = block == float(b), after == float(b)
                    for q in range(2 * count):
                        p, kind = q // 2, q % 2
                        level = levels[
                            p * N + b * 8 : p * N + b * 8 + 8,
                            (2 * chunk + kind) * LANES : (2 * chunk + kind + 1) * LANES,
                        ]
                        if b == 0:
                            near[q] = [level, level]
                        else:
                            near[q][0] = jnp.where(at, level, near[q][0])
                            near[q][1] = jnp.where(next_at, level, near[q][1])
                total = [jnp.zeros((8, LANES), jnp.float32) for _ in range(4)]
                for half in range(2):
                    along, along_dx = tiles[0][half], tiles[1][half]
                    plain = near[0][half] * row(30)
                    over_z = near[0][half] * row(32)
                    over_y = near[1][half] * row(30)
                    if count == 2:
                        plain = plain + near[2][half] * row(31)
                        over_z = over_z + near[2][half] * row(33)
                        over_y = over_y + near[3][half] * row(31)
                    total[0] = total[0] + along * plain
                    total[1] = total[1] + along_dx * plain
                    total[2] = total[2] + along * over_y
                    total[3] = total[3] + along * over_z
                total = [jnp.sum(t, axis=0, keepdims=True) for t in total]
                charge = ref[6, w : w + 1, lanes]
                for d in range(3):
                    out_ref[d, w : w + 1, lanes] = -charge * total[1 + d]
                energy = energy + charge * total[0]
                slope = slope + ref[7, w : w + 1, lanes] * total[0]
        sums[w : w + 1, :] = energy
        sums[WINDOWS + w : WINDOWS + w + 1, :] = slope
    added = jnp.sum(sums[...], axis=1, keepdims=True)
    shape = (8, LANES)
    here = lax.broadcasted_iota(jnp.int32, shape, 0) == lax.broadcasted_iota(jnp.int32, shape, 1)
    line = jnp.sum(jnp.where(here, added, 0.0), axis=0, keepdims=True)
    sum_out[...] = jnp.broadcast_to(line, (SLABS, LANES))


def finish_kernel(mine_ref, above_ref, far_ref, sum_ref, force_out, energy_out, slope_out):
    force_out[...] = mine_ref[...] + above_ref[...] + far_ref[...]
    line = jnp.sum(sum_ref[...], axis=0, keepdims=True)
    lane = lax.broadcasted_iota(jnp.int32, (1, LANES), 1)
    for w in range(WINDOWS):
        energy_out[w] = jnp.sum(jnp.where(lane == w, line, 0.0)) * (0.5 / ATOMS)
        slope_out[w] = jnp.sum(jnp.where(lane == WINDOWS + w, line, 0.0)) * (1.0 / ATOMS)


in_vmem = pl.BlockSpec(memory_space=pltpu.VMEM)
in_smem = pl.BlockSpec(memory_space=pltpu.SMEM)
in_hbm = pl.BlockSpec(memory_space=pltpu.HBM)
table_scratch = pltpu.VMEM((2, 2 * N, 2 * N), jnp.bfloat16)


def f32(*shape):
    return jax.ShapeDtypeStruct(shape, jnp.float32)


def run(kernel, out_shape, in_specs, operands, scratch=(), mib=16):
    several = isinstance(out_shape, tuple)
    return pl.pallas_call(
        kernel,
        out_shape=out_shape,
        in_specs=in_specs,
        out_specs=(in_vmem,) * len(out_shape) if several else in_vmem,
        scratch_shapes=list(scratch),
        compiler_params=pltpu.CompilerParams(vmem_limit_bytes=mib << 20),
        name=kernel.__name__,
    )(*operands)


def passed_along(value, steps):
    pairs = [(source, (source + steps) % SLABS) for source in range(SLABS)]
    return lax.ppermute(value, "slab", pairs)


def body(lambdas, charge_a, charge_b, perturbed, grid_index, spline_weights, spline_slopes):
    slab = lax.axis_index("slab").reshape(1)
    inputs = (lambdas, charge_a, charge_b, perturbed, grid_index, spline_weights)
    own = run(
        pack_kernel,
        f32(8, WINDOWS, HERE),
        [in_smem] + [in_hbm] * 6,
        (slab, *inputs),
        [pltpu.SMEM((WINDOWS,), jnp.float32)]
        + [pltpu.VMEM(a.shape, a.dtype) for a in inputs[1:]]
        + [pltpu.SemaphoreType.DMA((6,))],
        mib=60,
    )
    below = passed_along(own, 1)
    far = passed_along(own, 2)
    kept = lambda count, rows: pltpu.VMEM((count, rows, WINDOWS, HERE), jnp.float32)
    from_own, influence = run(
        own_spread_kernel,
        (f32(WINDOWS, N, 2 * N), f32(N, 4 * N)),
        [in_smem, in_vmem],
        (slab, own),
        [kept(1, 30)],
    )
    spectrum = run(
        spread_kernel,
        f32(2, N // 4, 2, 8, N),
        [in_vmem] * 3 + [in_hbm] * 2,
        (from_own, below, far, Y_FORWARD, X_FORWARD),
        [kept(2, 30), table_scratch, table_scratch, pltpu.SemaphoreType.DMA((2,))],
    )
    columns = lax.all_to_all(spectrum.reshape(SLABS, 16, N), "slab", 0, 0, tiled=True)
    columns = run(
        column_kernel,
        f32(8 * N, N),
        [in_vmem] * 4,
        (columns.reshape(8 * N, N), influence, Z_FORWARD, Z_INVERSE),
        mib=8,
    )
    levels = lax.all_to_all(columns.reshape(SLABS, 16, N), "slab", 0, 0, tiled=True)
    part = f32(3, WINDOWS, HERE)
    mine, for_below, for_far, sums = run(
        sample_kernel,
        (part, part, part, f32(SLABS, N)),
        [in_vmem] * 6,
        (levels.reshape(2, N // 4, 2, 8, N), own, below, far, X_INVERSE, Y_INVERSE),
        [kept(3, 34), pltpu.VMEM((8, LANES), jnp.float32)],
    )
    from_above = passed_along(for_below, -1)
    from_far = passed_along(for_far, -2)
    sums = lax.all_to_all(sums.reshape(SLABS, 1, N), "slab", 0, 0, tiled=True)
    return pl.pallas_call(
        finish_kernel,
        out_shape=(part, f32(WINDOWS), f32(WINDOWS)),
        in_specs=[in_vmem] * 4,
        out_specs=(in_vmem, in_smem, in_smem),
        compiler_params=pltpu.CompilerParams(vmem_limit_bytes=4 << 20),
        name="finish_kernel",
    )(mine, from_above, from_far, sums.reshape(SLABS, N))


def solution(mesh):
    return jax.shard_map(
        body,
        mesh=mesh,
        in_specs=(
            P("win"),
            P("win", "slab"),
            P("win", "slab"),
            P("win", "slab"),
            P(None, "win", "slab"),
            P(None, None, "win", "slab"),
            P(None, None, "win", "slab"),
        ),
        out_specs=(P(None, "win", "slab"), P("win"), P("win")),
        check_vma=False,
    )
```

```python
import math

import jax
import jax.numpy as jnp
import numpy as np
from jax import lax
from jax.experimental import pallas as pl
from jax.experimental.pallas import tpu as pltpu
from jax.sharding import PartitionSpec as P

N = 128
LANES = 128
WINDOWS = 4
HERE = 512
SLABS = 64
CHIPS = SLABS // 2
PAIR = WINDOWS // 2
DEEP = 4
ATOMS = SLABS * HERE
gauss_width = 2.0


def blocks(real, imaginary):
    return np.block([[real, -imaginary], [imaginary, real]])


def tables():
    k = np.arange(N)
    angle = 2.0 * np.pi * ((k[:, None] * k[None, :]) % N) / N
    cosine, sine = np.cos(angle), np.sin(angle)
    forward = blocks(cosine, -sine)
    inverse = blocks(cosine, sine)
    order = np.arange(2 * N).reshape(2, N // 4, 4).transpose(1, 0, 2).ravel()
    return tuple(
        np.ascontiguousarray(m, dtype=np.float32)
        for m in (
            forward.T,
            forward[order],
            forward,
            inverse,
            inverse[:, order],
            inverse.T,
        )
    )


def halves(x):
    top = x.astype(jnp.bfloat16)
    return top, (x - top.astype(jnp.float32)).astype(jnp.bfloat16)


def table_halves(table):
    top = table.astype(jnp.bfloat16)
    return np.stack([top, (table - top.astype(np.float32)).astype(jnp.bfloat16)])


Y_FORWARD, X_FORWARD, Z_FORWARD, Z_INVERSE, X_INVERSE, Y_INVERSE = map(table_halves, tables())


def dot(a, b, contract=(1, 0)):
    dims = (((contract[0],), (contract[1],)), ((), ()))
    return lax.dot_general(a, b, dims, preferred_element_type=jnp.float32)


def table_times(table_ref, x):
    top, rest = halves(x)
    return dot(table_ref[0], top) + dot(table_ref[1], top) + dot(table_ref[0], rest)


def times_table(x, table_ref):
    top, rest = halves(x)
    return dot(top, table_ref[0]) + dot(rest, table_ref[0]) + dot(top, table_ref[1])


def weights_of(u):
    v = 1.0 - u
    return (
        v * v * v * (1.0 / 6.0),
        (0.5 * u - 1.0) * u * u + (2.0 / 3.0),
        (0.5 * v - 1.0) * v * v + (2.0 / 3.0),
        u * u * u * (1.0 / 6.0),
    )


def slopes_of(u):
    v = 1.0 - u
    return (-0.5 * v * v, (1.5 * u - 2.0) * u, (2.0 - 1.5 * v) * v, 0.5 * u * u)


def pack_kernel(slab_ref, *refs):
    sources, (mine_ref, other_ref), landed, sem = refs[:6], refs[6:8], refs[8:14], refs[14]
    copies = [
        pltpu.make_async_copy(source, target, sem.at[i])
        for i, (source, target) in enumerate(zip(sources, landed))
    ]
    for copy in copies:
        copy.start()
    for copy in copies:
        copy.wait()
    lambda_ref, a_ref, b_ref, flag_ref, index_ref, weight_ref = landed
    flags = flag_ref[...].astype(jnp.float32)
    steps = flags * (b_ref[...] - a_ref[...])
    core = lax.rem(slab_ref[0], 2)
    first = (slab_ref[0] - core) * 2
    row = lax.broadcasted_iota(jnp.int32, (WINDOWS, HERE), 0)
    scale = jnp.zeros((WINDOWS, HERE), jnp.float32)
    for w in range(WINDOWS):
        scale = jnp.where(row == w, lambda_ref[w], scale)
    values = [
        index_ref[0].astype(jnp.float32),
        index_ref[1].astype(jnp.float32),
        (index_ref[2] - first).astype(jnp.float32),
    ]
    for axis in range(3):
        values.append(weight_ref[axis, 2] + 2.0 * weight_ref[axis, 3] - weight_ref[axis, 0])
    values += [a_ref[...] + scale * steps, steps]
    for r, value in enumerate(values):
        lower, upper = value[:PAIR], value[PAIR:]
        mine_ref[r] = jnp.where(core == 0, lower, upper)
        other_ref[r] = jnp.where(core == 0, upper, lower)


def places(first, height):
    block = jnp.floor(first * (1.0 / height))
    after = jnp.where(block == float(N // height - 1), 0.0, block + 1.0)
    return block, after, first - height * block


def row_halves(value):
    top = value.astype(jnp.bfloat16).astype(jnp.float32)
    return top, value - top


def wide(row):
    return jnp.broadcast_to(row, (16, LANES)).astype(jnp.bfloat16)


def tall(row):
    return jnp.broadcast_to(row, (8, LANES))


def rows_of(height):
    return lax.broadcasted_iota(jnp.int32, (height, LANES), 0).astype(jnp.float32)


def stencil_tiles(rows, height, start, columns):
    zero = jnp.zeros_like(rows)
    here = [rows == start + jnp.asarray(k, rows.dtype) for k in range(4)]
    past = [rows + jnp.asarray(height, rows.dtype) == start + jnp.asarray(k, rows.dtype) for k in range(1, 4)]
    tiles = []
    for values in columns:
        first = second = zero
        for k in range(4):
            first = jnp.where(here[k], values[k], first)
        for k in range(1, 4):
            second = jnp.where(past[k - 1], values[k], second)
        tiles.append((first, second))
    return tiles


def table_columns(block, after, tiles):
    columns = [[] for _ in tiles]
    zero = jnp.zeros_like(tiles[0][0])
    for b in range(N // 16):
        at, next_at = block == jnp.asarray(b, block.dtype), after == jnp.asarray(b, block.dtype)
        for column, (first, second) in zip(columns, tiles):
            column.append(jnp.where(at, first, jnp.where(next_at, second, zero)))
    return [jnp.concatenate(column, axis=0) for column in columns]


ANY, LOWER, UPPER, BELOW, FAR = range(5)
REACH = {ANY: (0, 4), LOWER: (0, 4), UPPER: (2, 4), BELOW: (0, 3), FAR: (0, 1)}


def plane_parts(kind, plane, parts):
    first, second, third, fourth = parts
    if kind == ANY:
        found = []
        for p in range(DEEP):
            value = 0.0
            for q in range(p + 1):
                value = jnp.where(plane == float(q), parts[p - q], value)
            found.append(value)
        return found
    low = plane < (0.5 if kind in (LOWER, FAR) else 2.5)
    if kind == LOWER:
        return [
            jnp.where(low, first, 0.0),
            jnp.where(low, second, first),
            jnp.where(low, third, second),
            jnp.where(low, fourth, third),
        ]
    if kind == UPPER:
        return [jnp.where(low, first, 0.0), jnp.where(low, second, first)]
    if kind == BELOW:
        return [
            jnp.where(low, third, second),
            jnp.where(low, fourth, third),
            jnp.where(low, 0.0, fourth),
        ]
    return [jnp.where(low, 0.0, fourth)]


def spread_rows(kind, rows, keep):
    block, after, row = places(rows[1], 16)
    keep[0], keep[1], keep[2] = block, after, row
    block, after, row = places(rows[0], 16)
    keep[3], keep[4], keep[5] = block, after, row
    for k, value in enumerate(weights_of(rows[4])):
        keep[6 + k], keep[10 + k] = row_halves(value)
    along_x = weights_of(rows[3])
    for p, depth in enumerate(plane_parts(kind, rows[2], weights_of(rows[5]))):
        for k in range(4):
            top, rest = row_halves(along_x[k] * (rows[6] * depth))
            keep[14 + 8 * p + k], keep[18 + 8 * p + k] = top, rest


def spread_planes(sources, keep, planes):
    for slot, (kind, rows) in enumerate(sources):
        spread_rows(kind, rows, keep.at[slot])
    rows16 = rows_of(16).astype(jnp.bfloat16)
    for w in range(PAIR):
        for slot, (kind, _) in enumerate(sources):
            start, stop = REACH[kind]
            count = stop - start
            left, right = [], []
            for chunk in range(HERE // LANES):
                lanes = slice(chunk * LANES, (chunk + 1) * LANES)
                row = lambda r: wide(keep[slot, r, w : w + 1, lanes])
                four = lambda r: [row(r + k) for k in range(4)]
                tiles = stencil_tiles(rows16, 16, row(2), [four(6), four(10)])
                right.append(jnp.concatenate(table_columns(row(0), row(1), tiles), axis=0))
                tiles = stencil_tiles(
                    rows16, 16, row(5), [four(14 + 4 * i) for i in range(2 * count)]
                )
                found = table_columns(row(3), row(4), tiles)
                left.append(jnp.concatenate(found[0::2] + found[1::2], axis=0))
            both = dot(jnp.concatenate(left, axis=1), jnp.concatenate(right, axis=1), (1, 1))
            height = count * N
            added = both[:height, :N] + both[:height, N:] + both[height:, :N]
            for p in range(count):
                part = added[p * N : p * N + N]
                known = planes[w][start + p]
                planes[w][start + p] = part if known is None else known + part
    return planes


def own_spread_kernel(slab_ref, own_ref, out_ref, influence_ref, keep):
    fill_influence(slab_ref, influence_ref)
    planes = [[None] * DEEP for _ in range(PAIR)]
    spread_planes([(ANY, [own_ref[r] for r in range(8)])], keep, planes)
    for w in range(PAIR):
        for p in range(DEEP):
            out_ref[w, p] = planes[w][p]


def by_core(core, first_ref, second_ref):
    pairs = [(first_ref[r], second_ref[r]) for r in range(8)]
    return (
        [jnp.where(core == 0, a, b) for a, b in pairs],
        [jnp.where(core == 0, b, a) for a, b in pairs],
    )


def spread_kernel(
    slab_ref, own_ref, near_ref, same_ref, cross_ref, y_hbm, x_hbm, out_ref, keep, y_ref, x_ref, sem
):
    copies = [
        pltpu.make_async_copy(y_hbm, y_ref, sem.at[0]),
        pltpu.make_async_copy(x_hbm, x_ref, sem.at[1]),
    ]
    for copy in copies:
        copy.start()
    core = lax.rem(slab_ref[0], 2)
    far, below = by_core(core, same_ref, cross_ref)
    planes = [[own_ref[w, p] for p in range(DEEP)] for w in range(PAIR)]
    near = [near_ref[r] for r in range(8)]
    spread_planes([(ANY, near), (BELOW, below), (FAR, far)], keep, planes)
    for copy in copies:
        copy.wait()
    stacked = jnp.concatenate(
        [jnp.concatenate([planes[0][p], planes[1][p]], axis=1) for p in range(DEEP)], axis=0
    )
    turned = times_table(stacked, y_ref)
    upright = jnp.concatenate(
        [
            jnp.concatenate([turned[b * N : b * N + N, :N], turned[b * N : b * N + N, N:]], axis=0)
            for b in range(DEEP)
        ],
        axis=1,
    )
    columns = table_times(x_ref, upright)
    for b in range(DEEP):
        out_ref[:, b] = columns[:, b * N : b * N + N].reshape(N // 4, 8, N)


def frequency(counter):
    return jnp.where(counter >= N // 2, counter - N, counter).astype(jnp.float32) / N


def fill_influence(slab_ref, out_ref):
    first = (slab_ref[0] - lax.rem(slab_ref[0], 2)) * 2
    shape = (N, N)
    freq_z = frequency(lax.broadcasted_iota(jnp.int32, shape, 0))
    freq_y = frequency(lax.broadcasted_iota(jnp.int32, shape, 1))
    flat = freq_z * freq_z + freq_y * freq_y
    for j in range(4):
        freq_x = frequency(jnp.full(shape, first + j, jnp.int32))
        squared = flat + freq_x * freq_x
        positive = squared > 0
        safe = jnp.where(positive, squared, 1.0)
        out_ref[:, j * N : j * N + N] = jnp.where(
            positive, jnp.exp(-gauss_width * squared) / (math.pi * N * N * N * safe), 0.0
        )


def column_kernel(in_ref, influence_ref, forward_ref, inverse_ref, out_ref):
    part = lambda r: in_ref[pl.ds(r, N, stride=8), :]
    columns = jnp.concatenate(
        [jnp.concatenate([part(j), part(4 + j)], axis=0) for j in range(4)], axis=1
    )
    depth = table_times(forward_ref, columns)
    influence = influence_ref[...]
    depth = jnp.concatenate([depth[:N] * influence, depth[N:] * influence], axis=0)
    back = table_times(inverse_ref, depth)
    for j in range(4):
        out_ref[pl.ds(j, N, stride=8), :] = back[:N, j * N : j * N + N]
        out_ref[pl.ds(4 + j, N, stride=8), :] = back[N:, j * N : j * N + N]


def sample_rows(kind, rows, keep):
    block, after, row = places(rows[1], 16)
    keep[0], keep[1], keep[2] = block, after, row
    for k, value in enumerate(weights_of(rows[4])):
        keep[3 + k], keep[7 + k] = row_halves(value)
    for k, value in enumerate(slopes_of(rows[4])):
        keep[11 + k], keep[15 + k] = row_halves(value)
    block, after, row = places(rows[0], 8)
    keep[19], keep[20], keep[21] = block, after, row
    for k, (value, slope) in enumerate(zip(weights_of(rows[3]), slopes_of(rows[3]))):
        keep[22 + k], keep[26 + k] = value, slope
    for p, depth in enumerate(plane_parts(kind, rows[2], weights_of(rows[5]))):
        keep[30 + p] = depth
    for p, steep in enumerate(plane_parts(kind, rows[2], slopes_of(rows[5]))):
        keep[34 + p] = steep
    keep[38], keep[39] = rows[6], rows[7]


def sample_kernel(
    slab_ref,
    in_ref,
    own_ref,
    near_ref,
    same_ref,
    cross_ref,
    x_ref,
    y_ref,
    own_out,
    near_out,
    same_out,
    cross_out,
    sum_out,
    keep,
    forces,
    sums,
):
    core = lax.rem(slab_ref[0], 2)
    columns = jnp.concatenate([in_ref[:, b].reshape(2 * N, N) for b in range(DEEP)], axis=1)
    upright = table_times(x_ref, columns)
    flat = jnp.concatenate(
        [
            jnp.concatenate([upright[:N, b * N : b * N + N], upright[N:, b * N : b * N + N]], axis=1)
            for b in range(DEEP)
        ],
        axis=0,
    )
    pairs = times_table(flat, y_ref)
    lower, upper = by_core(core, own_ref, near_ref)
    far, below = by_core(core, same_ref, cross_ref)
    sources = ((LOWER, lower), (UPPER, upper), (BELOW, below), (FAR, far))
    for slot, (kind, rows) in enumerate(sources):
        sample_rows(kind, rows, keep.at[slot])
    rows16 = rows_of(16).astype(jnp.bfloat16)
    rows8 = rows_of(8)
    for w in range(PAIR):
        planes = jnp.concatenate(halves(pairs[:, w * N : w * N + N]), axis=1)
        energy = jnp.zeros((1, LANES), jnp.float32)
        slope = jnp.zeros((1, LANES), jnp.float32)
        for slot, (kind, _) in enumerate(sources):
            start, stop = REACH[kind]
            count = stop - start
            tops, rests = [], []
            for chunk in range(HERE // LANES):
                lanes = slice(chunk * LANES, (chunk + 1) * LANES)
                row = lambda r: wide(keep[slot, r, w : w + 1, lanes])
                four = lambda r: [row(r + k) for k in range(4)]
                tiles = stencil_tiles(rows16, 16, row(2), [four(3 + 4 * i) for i in range(4)])
                found = table_columns(row(0), row(1), tiles)
                tops.append(jnp.concatenate([found[0], found[2]], axis=1))
                rests.append(jnp.concatenate([found[1], found[3]], axis=1))
            tops = jnp.concatenate(tops, axis=1)
            rests = jnp.concatenate(rests, axis=1)
            used = planes[start * N : stop * N]
            levels = dot(used, jnp.concatenate([tops, tops], axis=0)) + dot(used[:, :N], rests)
            for chunk in range(HERE // LANES):
                lanes = slice(chunk * LANES, (chunk + 1) * LANES)
                row = lambda r: tall(keep[slot, r, w : w + 1, lanes])
                four = lambda r: [row(r + k) for k in range(4)]
                block, after = row(19), row(20)
                tiles = stencil_tiles(rows8, 8, row(21), [four(22), four(26)])
                near = [[None] * 2 for _ in range(2 * count)]
                for b in range(N // 8):
                    at, next_at = block == float(b), after == float(b)
                    for q in range(2 * count):
                        p, slant = q // 2, q % 2
                        level = levels[
                            p * N + b * 8 : p * N + b * 8 + 8,
                            (2 * chunk + slant) * LANES : (2 * chunk + slant + 1) * LANES,
                        ]
                        if b == 0:
                            near[q] = [level, level]
                        else:
                            near[q][0] = jnp.where(at, level, near[q][0])
                            near[q][1] = jnp.where(next_at, level, near[q][1])
                total = [jnp.zeros((8, LANES), jnp.float32) for _ in range(4)]
                for half in range(2):
                    along, along_dx = tiles[0][half], tiles[1][half]
                    plain = near[0][half] * row(30)
                    over_z = near[0][half] * row(34)
                    over_y = near[1][half] * row(30)
                    for p in range(1, count):
                        plain = plain + near[2 * p][half] * row(30 + p)
                        over_z = over_z + near[2 * p][half] * row(34 + p)
                        over_y = over_y + near[2 * p + 1][half] * row(30 + p)
                    total[0] = total[0] + along * plain
                    total[1] = total[1] + along_dx * plain
                    total[2] = total[2] + along * over_y
                    total[3] = total[3] + along * over_z
                total = [jnp.sum(t, axis=0, keepdims=True) for t in total]
                charge = keep[slot, 38, w : w + 1, lanes]
                for d in range(3):
                    forces[slot, d, w : w + 1, lanes] = -charge * total[1 + d]
                energy = energy + charge * total[0]
                slope = slope + keep[slot, 39, w : w + 1, lanes] * total[0]
        sums[w : w + 1, :] = energy
        sums[PAIR + w : PAIR + w + 1, :] = slope
    own_out[...] = jnp.where(core == 0, forces[0], forces[1])
    near_out[...] = jnp.where(core == 0, forces[1], forces[0])
    same_out[...] = jnp.where(core == 0, forces[3], forces[2])
    cross_out[...] = jnp.where(core == 0, forces[2], forces[3])
    added = jnp.sum(sums[...], axis=1, keepdims=True)
    shape = (2 * PAIR, LANES)
    row = lax.broadcasted_iota(jnp.int32, shape, 0)
    place = PAIR * core + jnp.where(row < PAIR, row, row - PAIR + WINDOWS)
    here = lax.broadcasted_iota(jnp.int32, shape, 1) == place
    line = jnp.sum(jnp.where(here, added, 0.0), axis=0, keepdims=True)
    sum_out[...] = jnp.broadcast_to(line, (SLABS, LANES))


def finish_kernel(
    slab_ref, own_ref, near_ref, same_ref, cross_ref, sum_ref, force_out, energy_out, slope_out
):
    core = lax.rem(slab_ref[0], 2)
    mine = own_ref[...] + same_ref[...]
    other = near_ref[...] + cross_ref[...]
    force_out[:, :PAIR] = jnp.where(core == 0, mine, other)
    force_out[:, PAIR:] = jnp.where(core == 0, other, mine)
    line = jnp.sum(sum_ref[...], axis=0, keepdims=True)
    lane = lax.broadcasted_iota(jnp.int32, (1, LANES), 1)
    for w in range(WINDOWS):
        energy_out[w] = jnp.sum(jnp.where(lane == w, line, 0.0)) * (0.5 / ATOMS)
        slope_out[w] = jnp.sum(jnp.where(lane == WINDOWS + w, line, 0.0)) * (1.0 / ATOMS)


in_vmem = pl.BlockSpec(memory_space=pltpu.VMEM)
in_smem = pl.BlockSpec(memory_space=pltpu.SMEM)
in_hbm = pl.BlockSpec(memory_space=pltpu.HBM)
table_scratch = pltpu.VMEM((2, 2 * N, 2 * N), jnp.bfloat16)


def far_away(array):
    return pltpu.with_memory_space_constraint(array, pltpu.HBM)


def f32(*shape):
    return jax.ShapeDtypeStruct(shape, jnp.float32)


def run(kernel, out_shape, in_specs, operands, scratch=(), mib=16):
    several = isinstance(out_shape, tuple)
    return pl.pallas_call(
        kernel,
        out_shape=out_shape,
        in_specs=in_specs,
        out_specs=(in_vmem,) * len(out_shape) if several else in_vmem,
        scratch_shapes=list(scratch),
        compiler_params=pltpu.CompilerParams(vmem_limit_bytes=mib << 20),
        name=kernel.__name__,
    )(*operands)


def moved(value, pairs, back=False):
    return lax.ppermute(value, "slab", [pair[::-1] if back else pair for pair in pairs])


TO_PARTNER = [(d, d ^ 1) for d in range(SLABS)]
UP_SAME = [(d, (d + 2) % SLABS) for d in range(SLABS)]
UP_CROSS = [(d, ((d ^ 1) + 2) % SLABS) for d in range(SLABS)]
CORES = [list(range(c, SLABS, 2)) for c in range(2)]


def exchanged(value):
    return lax.all_to_all(value, "slab", 0, 0, tiled=True, axis_index_groups=CORES)


def body(lambdas, charge_a, charge_b, perturbed, grid_index, spline_weights, spline_slopes):
    slab = lax.axis_index("slab").reshape(1)
    inputs = tuple(
        far_away(a)
        for a in (lambdas, charge_a, charge_b, perturbed, grid_index, spline_weights)
    )
    atoms = f32(8, PAIR, HERE)
    own, other = run(
        pack_kernel,
        (atoms, atoms),
        [in_smem] + [in_hbm] * 6,
        (slab, *inputs),
        [pltpu.SMEM((WINDOWS,), jnp.float32)]
        + [pltpu.VMEM(a.shape, a.dtype) for a in inputs[1:]]
        + [pltpu.SemaphoreType.DMA((6,))],
        mib=4,
    )
    near = moved(other, TO_PARTNER)
    same = moved(own, UP_SAME)
    cross = moved(other, UP_CROSS)
    kept = lambda count, rows: pltpu.VMEM((count, rows, PAIR, HERE), jnp.float32)
    from_own, influence = run(
        own_spread_kernel,
        (f32(PAIR, DEEP, N, N), f32(N, 4 * N)),
        [in_smem, in_vmem],
        (slab, own),
        [kept(1, 46)],
    )
    spectrum = run(
        spread_kernel,
        f32(CHIPS, DEEP, 8, N),
        [in_smem] + [in_vmem] * 4 + [in_hbm] * 2,
        (
            slab,
            from_own,
            near,
            same,
            cross,
            far_away(jnp.asarray(Y_FORWARD)),
            far_away(jnp.asarray(X_FORWARD)),
        ),
        [kept(3, 46), table_scratch, table_scratch, pltpu.SemaphoreType.DMA((2,))],
    )
    columns = exchanged(spectrum.reshape(CHIPS, 8 * DEEP, N))
    columns = run(
        column_kernel,
        f32(8 * N, N),
        [in_vmem] * 4,
        (columns.reshape(8 * N, N), influence, Z_FORWARD, Z_INVERSE),
        mib=8,
    )
    levels = exchanged(columns.reshape(CHIPS, 8 * DEEP, N))
    part = f32(3, PAIR, HERE)
    mine, for_near, for_same, for_cross, sums = run(
        sample_kernel,
        (part, part, part, part, f32(SLABS, N)),
        [in_smem] + [in_vmem] * 7,
        (slab, levels.reshape(CHIPS, DEEP, 8, N), own, near, same, cross, X_INVERSE, Y_INVERSE),
        [
            kept(4, 40),
            pltpu.VMEM((4, 3, PAIR, HERE), jnp.float32),
            pltpu.VMEM((2 * PAIR, LANES), jnp.float32),
        ],
    )
    from_near = moved(for_near, TO_PARTNER, back=True)
    from_same = moved(for_same, UP_SAME, back=True)
    from_cross = moved(for_cross, UP_CROSS, back=True)
    sums = lax.all_to_all(sums.reshape(SLABS, 1, N), "slab", 0, 0, tiled=True)
    return pl.pallas_call(
        finish_kernel,
        out_shape=(f32(3, WINDOWS, HERE), f32(WINDOWS), f32(WINDOWS)),
        in_specs=[in_smem] + [in_vmem] * 5,
        out_specs=(in_vmem, in_smem, in_smem),
        compiler_params=pltpu.CompilerParams(vmem_limit_bytes=4 << 20),
        name="finish_kernel",
    )(slab, mine, from_near, from_same, from_cross, sums.reshape(SLABS, N))


def solution(mesh):
    return jax.shard_map(
        body,
        mesh=mesh,
        in_specs=(
            P("win"),
            P("win", "slab"),
            P("win", "slab"),
            P("win", "slab"),
            P(None, "win", "slab"),
            P(None, None, "win", "slab"),
            P(None, None, "win", "slab"),
        ),
        out_specs=(P(None, "win", "slab"), P("win"), P("win")),
        check_vma=False,
    )
```

```python
import math

import jax
import jax.numpy as jnp
import numpy as np
from jax import lax
from jax.experimental import pallas as pl
from jax.experimental.pallas import tpu as pltpu
from jax.sharding import PartitionSpec as P

N = 128
LANES = 128
WINDOWS = 4
HERE = 512
SLABS = 64
CHIPS = SLABS // 2
PAIR = WINDOWS // 2
DEEP = 4
ATOMS = SLABS * HERE
gauss_width = 2.0


def blocks(real, imaginary):
    return np.block([[real, -imaginary], [imaginary, real]])


def tables():
    k = np.arange(N)
    angle = 2.0 * np.pi * ((k[:, None] * k[None, :]) % N) / N
    cosine, sine = np.cos(angle), np.sin(angle)
    forward = blocks(cosine, -sine)
    inverse = blocks(cosine, sine)
    order = np.arange(2 * N).reshape(2, N // 4, 4).transpose(1, 0, 2).ravel()
    return tuple(
        np.ascontiguousarray(m, dtype=np.float32)
        for m in (
            forward.T,
            forward[order],
            forward,
            inverse,
            inverse[:, order],
            inverse.T,
        )
    )


def halves(x):
    top = x.astype(jnp.bfloat16)
    return top, (x - top.astype(jnp.float32)).astype(jnp.bfloat16)


def table_halves(table):
    top = table.astype(jnp.bfloat16)
    return np.stack([top, (table - top.astype(np.float32)).astype(jnp.bfloat16)])


Y_FORWARD, X_FORWARD, Z_FORWARD, Z_INVERSE, X_INVERSE, Y_INVERSE = map(table_halves, tables())


def dot(a, b, contract=(1, 0)):
    dims = (((contract[0],), (contract[1],)), ((), ()))
    return lax.dot_general(a, b, dims, preferred_element_type=jnp.float32)


def table_times(table_ref, x):
    top, rest = halves(x)
    return dot(table_ref[0], top) + dot(table_ref[1], top) + dot(table_ref[0], rest)


def times_table(x, table_ref):
    top, rest = halves(x)
    return dot(top, table_ref[0]) + dot(rest, table_ref[0]) + dot(top, table_ref[1])


def weights_of(u):
    v = 1.0 - u
    return (
        v * v * v * (1.0 / 6.0),
        (0.5 * u - 1.0) * u * u + (2.0 / 3.0),
        (0.5 * v - 1.0) * v * v + (2.0 / 3.0),
        u * u * u * (1.0 / 6.0),
    )


def slopes_of(u):
    v = 1.0 - u
    return (-0.5 * v * v, (1.5 * u - 2.0) * u, (2.0 - 1.5 * v) * v, 0.5 * u * u)


def pack_kernel(*refs):
    slab = lax.axis_index("slab")
    sources, (mine_ref, other_ref), landed, sem = refs[:6], refs[6:8], refs[8:14], refs[14]
    copies = [
        pltpu.make_async_copy(source, target, sem.at[i])
        for i, (source, target) in enumerate(zip(sources, landed))
    ]
    for copy in copies:
        copy.start()
    for copy in copies:
        copy.wait()
    lambda_ref, a_ref, b_ref, flag_ref, index_ref, weight_ref = landed
    flags = flag_ref[...].astype(jnp.float32)
    steps = flags * (b_ref[...] - a_ref[...])
    core = lax.rem(slab, 2)
    first = (slab - core) * 2
    row = lax.broadcasted_iota(jnp.int32, (WINDOWS, HERE), 0)
    scale = jnp.zeros((WINDOWS, HERE), jnp.float32)
    for w in range(WINDOWS):
        scale = jnp.where(row == w, lambda_ref[w], scale)
    values = [
        index_ref[0].astype(jnp.float32),
        index_ref[1].astype(jnp.float32),
        (index_ref[2] - first).astype(jnp.float32),
    ]
    for axis in range(3):
        values.append(weight_ref[axis, 2] + 2.0 * weight_ref[axis, 3] - weight_ref[axis, 0])
    values += [a_ref[...] + scale * steps, steps]
    for r, value in enumerate(values):
        lower, upper = value[:PAIR], value[PAIR:]
        mine_ref[r] = jnp.where(core == 0, lower, upper)
        other_ref[r] = jnp.where(core == 0, upper, lower)


def places(first, height):
    block = jnp.floor(first * (1.0 / height))
    after = jnp.where(block == float(N // height - 1), 0.0, block + 1.0)
    return block, after, first - height * block


def row_halves(value):
    top = value.astype(jnp.bfloat16).astype(jnp.float32)
    return top, value - top


def wide(row):
    return jnp.broadcast_to(row, (16, LANES)).astype(jnp.bfloat16)


def tall(row):
    return jnp.broadcast_to(row, (8, LANES))


def rows_of(height):
    return lax.broadcasted_iota(jnp.int32, (height, LANES), 0).astype(jnp.float32)


def stencil_tiles(rows, height, start, columns):
    zero = jnp.zeros_like(rows)
    here = [rows == start + jnp.asarray(k, rows.dtype) for k in range(4)]
    past = [rows + jnp.asarray(height, rows.dtype) == start + jnp.asarray(k, rows.dtype) for k in range(1, 4)]
    tiles = []
    for values in columns:
        first = second = zero
        for k in range(4):
            first = jnp.where(here[k], values[k], first)
        for k in range(1, 4):
            second = jnp.where(past[k - 1], values[k], second)
        tiles.append((first, second))
    return tiles


def table_columns(block, after, tiles):
    columns = [[] for _ in tiles]
    zero = jnp.zeros_like(tiles[0][0])
    for b in range(N // 16):
        at, next_at = block == jnp.asarray(b, block.dtype), after == jnp.asarray(b, block.dtype)
        for column, (first, second) in zip(columns, tiles):
            column.append(jnp.where(at, first, jnp.where(next_at, second, zero)))
    return [jnp.concatenate(column, axis=0) for column in columns]


ANY, LOWER, UPPER, BELOW, FAR = range(5)
REACH = {ANY: (0, 4), LOWER: (0, 4), UPPER: (2, 4), BELOW: (0, 3), FAR: (0, 1)}


def plane_parts(kind, plane, parts):
    first, second, third, fourth = parts
    if kind == ANY:
        found = []
        for p in range(DEEP):
            value = 0.0
            for q in range(p + 1):
                value = jnp.where(plane == float(q), parts[p - q], value)
            found.append(value)
        return found
    low = plane < (0.5 if kind in (LOWER, FAR) else 2.5)
    if kind == LOWER:
        return [
            jnp.where(low, first, 0.0),
            jnp.where(low, second, first),
            jnp.where(low, third, second),
            jnp.where(low, fourth, third),
        ]
    if kind == UPPER:
        return [jnp.where(low, first, 0.0), jnp.where(low, second, first)]
    if kind == BELOW:
        return [
            jnp.where(low, third, second),
            jnp.where(low, fourth, third),
            jnp.where(low, 0.0, fourth),
        ]
    return [jnp.where(low, 0.0, fourth)]


def spread_rows(kind, rows, keep):
    block, after, row = places(rows[1], 16)
    keep[0], keep[1], keep[2] = block, after, row
    block, after, row = places(rows[0], 16)
    keep[3], keep[4], keep[5] = block, after, row
    for k, value in enumerate(weights_of(rows[4])):
        keep[6 + k], keep[10 + k] = row_halves(value)
    along_x = weights_of(rows[3])
    for p, depth in enumerate(plane_parts(kind, rows[2], weights_of(rows[5]))):
        for k in range(4):
            top, rest = row_halves(along_x[k] * (rows[6] * depth))
            keep[14 + 8 * p + k], keep[18 + 8 * p + k] = top, rest


def spread_planes(sources, keep, planes):
    for slot, (kind, rows) in enumerate(sources):
        spread_rows(kind, rows, keep.at[slot])
    rows16 = rows_of(16).astype(jnp.bfloat16)
    for w in range(PAIR):
        for slot, (kind, _) in enumerate(sources):
            start, stop = REACH[kind]
            count = stop - start
            left, right = [], []
            for chunk in range(HERE // LANES):
                lanes = slice(chunk * LANES, (chunk + 1) * LANES)
                row = lambda r: wide(keep[slot, r, w : w + 1, lanes])
                four = lambda r: [row(r + k) for k in range(4)]
                tiles = stencil_tiles(rows16, 16, row(2), [four(6), four(10)])
                right.append(jnp.concatenate(table_columns(row(0), row(1), tiles), axis=0))
                tiles = stencil_tiles(
                    rows16, 16, row(5), [four(14 + 4 * i) for i in range(2 * count)]
                )
                found = table_columns(row(3), row(4), tiles)
                left.append(jnp.concatenate(found[0::2] + found[1::2], axis=0))
            both = dot(jnp.concatenate(left, axis=1), jnp.concatenate(right, axis=1), (1, 1))
            height = count * N
            added = both[:height, :N] + both[:height, N:] + both[height:, :N]
            for p in range(count):
                part = added[p * N : p * N + N]
                known = planes[w][start + p]
                planes[w][start + p] = part if known is None else known + part
    return planes


def chip_spread_kernel(own_ref, near_ref, out_ref, influence_ref, keep):
    fill_influence(influence_ref)
    planes = [[None] * DEEP for _ in range(PAIR)]
    here = [(ANY, [ref[r] for r in range(8)]) for ref in (own_ref, near_ref)]
    spread_planes(here, keep, planes)
    for w in range(PAIR):
        for p in range(DEEP):
            out_ref[w, p] = planes[w][p]


def by_core(core, first_ref, second_ref):
    pairs = [(first_ref[r], second_ref[r]) for r in range(8)]
    return (
        [jnp.where(core == 0, a, b) for a, b in pairs],
        [jnp.where(core == 0, b, a) for a, b in pairs],
    )


def spread_kernel(
    chip_ref, same_ref, cross_ref, y_hbm, x_hbm, out_ref, keep, y_ref, x_ref, sem
):
    copies = [
        pltpu.make_async_copy(y_hbm, y_ref, sem.at[0]),
        pltpu.make_async_copy(x_hbm, x_ref, sem.at[1]),
    ]
    for copy in copies:
        copy.start()
    core = lax.rem(lax.axis_index("slab"), 2)
    far, below = by_core(core, same_ref, cross_ref)
    planes = [[chip_ref[w, p] for p in range(DEEP)] for w in range(PAIR)]
    spread_planes([(BELOW, below), (FAR, far)], keep, planes)
    for copy in copies:
        copy.wait()
    stacked = jnp.concatenate(
        [jnp.concatenate([planes[0][p], planes[1][p]], axis=1) for p in range(DEEP)], axis=0
    )
    turned = times_table(stacked, y_ref)
    upright = jnp.concatenate(
        [
            jnp.concatenate([turned[b * N : b * N + N, :N], turned[b * N : b * N + N, N:]], axis=0)
            for b in range(DEEP)
        ],
        axis=1,
    )
    columns = table_times(x_ref, upright)
    for b in range(DEEP):
        out_ref[:, b] = columns[:, b * N : b * N + N].reshape(N // 4, 8, N)


def frequency(counter):
    return jnp.where(counter >= N // 2, counter - N, counter).astype(jnp.float32) / N


def fill_influence(out_ref):
    slab = lax.axis_index("slab")
    first = (slab - lax.rem(slab, 2)) * 2
    shape = (N, N)
    freq_z = frequency(lax.broadcasted_iota(jnp.int32, shape, 0))
    freq_y = frequency(lax.broadcasted_iota(jnp.int32, shape, 1))
    flat = freq_z * freq_z + freq_y * freq_y
    for j in range(4):
        freq_x = frequency(jnp.full(shape, first + j, jnp.int32))
        squared = flat + freq_x * freq_x
        positive = squared > 0
        safe = jnp.where(positive, squared, 1.0)
        out_ref[:, j * N : j * N + N] = jnp.where(
            positive, jnp.exp(-gauss_width * squared) / (math.pi * N * N * N * safe), 0.0
        )


def column_kernel(in_ref, influence_ref, forward_ref, inverse_ref, out_ref):
    part = lambda r: in_ref[pl.ds(r, N, stride=8), :]
    columns = jnp.concatenate(
        [jnp.concatenate([part(j), part(4 + j)], axis=0) for j in range(4)], axis=1
    )
    depth = table_times(forward_ref, columns)
    influence = influence_ref[...]
    depth = jnp.concatenate([depth[:N] * influence, depth[N:] * influence], axis=0)
    back = table_times(inverse_ref, depth)
    for j in range(4):
        out_ref[pl.ds(j, N, stride=8), :] = back[:N, j * N : j * N + N]
        out_ref[pl.ds(4 + j, N, stride=8), :] = back[N:, j * N : j * N + N]


def sample_rows(kind, rows, keep):
    block, after, row = places(rows[1], 16)
    keep[0], keep[1], keep[2] = block, after, row
    for k, value in enumerate(weights_of(rows[4])):
        keep[3 + k], keep[7 + k] = row_halves(value)
    for k, value in enumerate(slopes_of(rows[4])):
        keep[11 + k], keep[15 + k] = row_halves(value)
    block, after, row = places(rows[0], 8)
    keep[19], keep[20], keep[21] = block, after, row
    for k, (value, slope) in enumerate(zip(weights_of(rows[3]), slopes_of(rows[3]))):
        keep[22 + k], keep[26 + k] = value, slope
    for p, depth in enumerate(plane_parts(kind, rows[2], weights_of(rows[5]))):
        keep[30 + p] = depth
    for p, steep in enumerate(plane_parts(kind, rows[2], slopes_of(rows[5]))):
        keep[34 + p] = steep
    keep[38], keep[39] = rows[6], rows[7]


def sample_kernel(
    in_ref,
    own_ref,
    near_ref,
    same_ref,
    cross_ref,
    x_ref,
    y_ref,
    own_out,
    near_out,
    same_out,
    cross_out,
    sum_out,
    keep,
    forces,
    sums,
):
    core = lax.rem(lax.axis_index("slab"), 2)
    columns = jnp.concatenate([in_ref[:, b].reshape(2 * N, N) for b in range(DEEP)], axis=1)
    upright = table_times(x_ref, columns)
    flat = jnp.concatenate(
        [
            jnp.concatenate([upright[:N, b * N : b * N + N], upright[N:, b * N : b * N + N]], axis=1)
            for b in range(DEEP)
        ],
        axis=0,
    )
    pairs = times_table(flat, y_ref)
    lower, upper = by_core(core, own_ref, near_ref)
    far, below = by_core(core, same_ref, cross_ref)
    sources = ((LOWER, lower), (UPPER, upper), (BELOW, below), (FAR, far))
    for slot, (kind, rows) in enumerate(sources):
        sample_rows(kind, rows, keep.at[slot])
    rows16 = rows_of(16).astype(jnp.bfloat16)
    rows8 = rows_of(8)
    for w in range(PAIR):
        planes = jnp.concatenate(halves(pairs[:, w * N : w * N + N]), axis=1)
        energy = jnp.zeros((1, LANES), jnp.float32)
        slope = jnp.zeros((1, LANES), jnp.float32)
        for slot, (kind, _) in enumerate(sources):
            start, stop = REACH[kind]
            count = stop - start
            tops, rests = [], []
            for chunk in range(HERE // LANES):
                lanes = slice(chunk * LANES, (chunk + 1) * LANES)
                row = lambda r: wide(keep[slot, r, w : w + 1, lanes])
                four = lambda r: [row(r + k) for k in range(4)]
                tiles = stencil_tiles(rows16, 16, row(2), [four(3 + 4 * i) for i in range(4)])
                found = table_columns(row(0), row(1), tiles)
                tops.append(jnp.concatenate([found[0], found[2]], axis=1))
                rests.append(jnp.concatenate([found[1], found[3]], axis=1))
            tops = jnp.concatenate(tops, axis=1)
            rests = jnp.concatenate(rests, axis=1)
            used = planes[start * N : stop * N]
            levels = dot(used, jnp.concatenate([tops, tops], axis=0)) + dot(used[:, :N], rests)
            for chunk in range(HERE // LANES):
                lanes = slice(chunk * LANES, (chunk + 1) * LANES)
                row = lambda r: tall(keep[slot, r, w : w + 1, lanes])
                four = lambda r: [row(r + k) for k in range(4)]
                block, after = row(19), row(20)
                tiles = stencil_tiles(rows8, 8, row(21), [four(22), four(26)])
                near = [[None] * 2 for _ in range(2 * count)]
                for b in range(N // 8):
                    at, next_at = block == float(b), after == float(b)
                    for q in range(2 * count):
                        p, slant = q // 2, q % 2
                        level = levels[
                            p * N + b * 8 : p * N + b * 8 + 8,
                            (2 * chunk + slant) * LANES : (2 * chunk + slant + 1) * LANES,
                        ]
                        if b == 0:
                            near[q] = [level, level]
                        else:
                            near[q][0] = jnp.where(at, level, near[q][0])
                            near[q][1] = jnp.where(next_at, level, near[q][1])
                total = [jnp.zeros((8, LANES), jnp.float32) for _ in range(4)]
                for half in range(2):
                    along, along_dx = tiles[0][half], tiles[1][half]
                    plain = near[0][half] * row(30)
                    over_z = near[0][half] * row(34)
                    over_y = near[1][half] * row(30)
                    for p in range(1, count):
                        plain = plain + near[2 * p][half] * row(30 + p)
                        over_z = over_z + near[2 * p][half] * row(34 + p)
                        over_y = over_y + near[2 * p + 1][half] * row(30 + p)
                    total[0] = total[0] + along * plain
                    total[1] = total[1] + along_dx * plain
                    total[2] = total[2] + along * over_y
                    total[3] = total[3] + along * over_z
                total = [jnp.sum(t, axis=0, keepdims=True) for t in total]
                charge = keep[slot, 38, w : w + 1, lanes]
                for d in range(3):
                    forces[slot, d, w : w + 1, lanes] = -charge * total[1 + d]
                energy = energy + charge * total[0]
                slope = slope + keep[slot, 39, w : w + 1, lanes] * total[0]
        sums[w : w + 1, :] = energy
        sums[PAIR + w : PAIR + w + 1, :] = slope
    own_out[...] = jnp.where(core == 0, forces[0], forces[1])
    near_out[...] = jnp.where(core == 0, forces[1], forces[0])
    same_out[...] = jnp.where(core == 0, forces[3], forces[2])
    cross_out[...] = jnp.where(core == 0, forces[2], forces[3])
    added = jnp.sum(sums[...], axis=1, keepdims=True)
    shape = (2 * PAIR, LANES)
    row = lax.broadcasted_iota(jnp.int32, shape, 0)
    place = PAIR * core + jnp.where(row < PAIR, row, row - PAIR + WINDOWS)
    here = lax.broadcasted_iota(jnp.int32, shape, 1) == place
    line = jnp.sum(jnp.where(here, added, 0.0), axis=0, keepdims=True)
    sum_out[...] = jnp.broadcast_to(line, (SLABS, LANES))


def finish_kernel(
    own_ref, near_ref, same_ref, cross_ref, sum_ref, force_out, energy_out, slope_out
):
    core = lax.rem(lax.axis_index("slab"), 2)
    mine = own_ref[...] + same_ref[...]
    other = near_ref[...] + cross_ref[...]
    force_out[:, :PAIR] = jnp.where(core == 0, mine, other)
    force_out[:, PAIR:] = jnp.where(core == 0, other, mine)
    line = jnp.sum(sum_ref[...], axis=0, keepdims=True)
    lane = lax.broadcasted_iota(jnp.int32, (1, LANES), 1)
    for w in range(WINDOWS):
        energy_out[w] = jnp.sum(jnp.where(lane == w, line, 0.0)) * (0.5 / ATOMS)
        slope_out[w] = jnp.sum(jnp.where(lane == WINDOWS + w, line, 0.0)) * (1.0 / ATOMS)


in_vmem = pl.BlockSpec(memory_space=pltpu.VMEM)
in_smem = pl.BlockSpec(memory_space=pltpu.SMEM)
in_hbm = pl.BlockSpec(memory_space=pltpu.HBM)
table_scratch = pltpu.VMEM((2, 2 * N, 2 * N), jnp.bfloat16)


def far_away(array):
    return pltpu.with_memory_space_constraint(array, pltpu.HBM)


def f32(*shape):
    return jax.ShapeDtypeStruct(shape, jnp.float32)


def run(kernel, out_shape, in_specs, operands, scratch=(), mib=16):
    several = isinstance(out_shape, tuple)
    return pl.pallas_call(
        kernel,
        out_shape=out_shape,
        in_specs=in_specs,
        out_specs=(in_vmem,) * len(out_shape) if several else in_vmem,
        scratch_shapes=list(scratch),
        compiler_params=pltpu.CompilerParams(vmem_limit_bytes=mib << 20),
        name=kernel.__name__,
    )(*operands)


def moved(value, pairs, back=False):
    return lax.ppermute(value, "slab", [pair[::-1] if back else pair for pair in pairs])


TO_PARTNER = [(d, d ^ 1) for d in range(SLABS)]
UP_SAME = [(d, (d + 2) % SLABS) for d in range(SLABS)]
UP_CROSS = [(d, ((d ^ 1) + 2) % SLABS) for d in range(SLABS)]
CORES = [list(range(c, SLABS, 2)) for c in range(2)]


def exchanged(value):
    return lax.all_to_all(value, "slab", 0, 0, tiled=True, axis_index_groups=CORES)


def body(lambdas, charge_a, charge_b, perturbed, grid_index, spline_weights, spline_slopes):
    inputs = tuple(
        far_away(a)
        for a in (lambdas, charge_a, charge_b, perturbed, grid_index, spline_weights)
    )
    atoms = f32(8, PAIR, HERE)
    own, other = run(
        pack_kernel,
        (atoms, atoms),
        [in_hbm] * 6,
        inputs,
        [pltpu.SMEM((WINDOWS,), jnp.float32)]
        + [pltpu.VMEM(a.shape, a.dtype) for a in inputs[1:]]
        + [pltpu.SemaphoreType.DMA((6,))],
        mib=4,
    )
    near = moved(other, TO_PARTNER)
    same = moved(own, UP_SAME)
    cross = moved(other, UP_CROSS)
    kept = lambda count, rows: pltpu.VMEM((count, rows, PAIR, HERE), jnp.float32)
    from_chip, influence = run(
        chip_spread_kernel,
        (f32(PAIR, DEEP, N, N), f32(N, 4 * N)),
        [in_vmem] * 2,
        (own, near),
        [kept(2, 46)],
    )
    spectrum = run(
        spread_kernel,
        f32(CHIPS, DEEP, 8, N),
        [in_vmem] * 3 + [in_hbm] * 2,
        (
            from_chip,
            same,
            cross,
            far_away(jnp.asarray(Y_FORWARD)),
            far_away(jnp.asarray(X_FORWARD)),
        ),
        [kept(2, 46), table_scratch, table_scratch, pltpu.SemaphoreType.DMA((2,))],
    )
    columns = exchanged(spectrum.reshape(CHIPS, 8 * DEEP, N))
    columns = run(
        column_kernel,
        f32(8 * N, N),
        [in_vmem] * 4,
        (columns.reshape(8 * N, N), influence, Z_FORWARD, Z_INVERSE),
        mib=8,
    )
    levels = exchanged(columns.reshape(CHIPS, 8 * DEEP, N))
    part = f32(3, PAIR, HERE)
    mine, for_near, for_same, for_cross, sums = run(
        sample_kernel,
        (part, part, part, part, f32(SLABS, N)),
        [in_vmem] * 7,
        (levels.reshape(CHIPS, DEEP, 8, N), own, near, same, cross, X_INVERSE, Y_INVERSE),
        [
            kept(4, 40),
            pltpu.VMEM((4, 3, PAIR, HERE), jnp.float32),
            pltpu.VMEM((2 * PAIR, LANES), jnp.float32),
        ],
    )
    from_near = moved(for_near, TO_PARTNER, back=True)
    from_same = moved(for_same, UP_SAME, back=True)
    from_cross = moved(for_cross, UP_CROSS, back=True)
    sums = lax.all_to_all(sums.reshape(SLABS, 1, N), "slab", 0, 0, tiled=True)
    return pl.pallas_call(
        finish_kernel,
        out_shape=(f32(3, WINDOWS, HERE), f32(WINDOWS), f32(WINDOWS)),
        in_specs=[in_vmem] * 5,
        out_specs=(in_vmem, in_smem, in_smem),
        compiler_params=pltpu.CompilerParams(vmem_limit_bytes=4 << 20),
        name="finish_kernel",
    )(mine, from_near, from_same, from_cross, sums.reshape(SLABS, N))


def solution(mesh):
    return jax.shard_map(
        body,
        mesh=mesh,
        in_specs=(
            P("win"),
            P("win", "slab"),
            P("win", "slab"),
            P("win", "slab"),
            P(None, "win", "slab"),
            P(None, None, "win", "slab"),
            P(None, None, "win", "slab"),
        ),
        out_specs=(P(None, "win", "slab"), P("win"), P("win")),
        check_vma=False,
    )
```

```python
import math

import jax
import jax.numpy as jnp
import numpy as np
from jax import lax
from jax.experimental import pallas as pl
from jax.experimental.pallas import tpu as pltpu
from jax.sharding import PartitionSpec as P

N = 128
LANES = 128
WINDOWS = 4
HERE = 512
SLABS = 64
CHIPS = SLABS // 2
PAIR = WINDOWS // 2
DEEP = 4
ATOMS = SLABS * HERE
gauss_width = 2.0


def blocks(real, imaginary):
    return np.block([[real, -imaginary], [imaginary, real]])


def tables():
    k = np.arange(N)
    angle = 2.0 * np.pi * ((k[:, None] * k[None, :]) % N) / N
    cosine, sine = np.cos(angle), np.sin(angle)
    forward = blocks(cosine, -sine)
    inverse = blocks(cosine, sine)
    order = np.arange(2 * N).reshape(2, N // 4, 4).transpose(1, 0, 2).ravel()
    return tuple(
        np.ascontiguousarray(m, dtype=np.float32)
        for m in (
            forward.T,
            forward[order],
            forward,
            inverse,
            inverse[:, order],
            inverse.T,
        )
    )


def halves(x):
    top = x.astype(jnp.bfloat16)
    return top, (x - top.astype(jnp.float32)).astype(jnp.bfloat16)


def table_halves(table):
    top = table.astype(jnp.bfloat16)
    return np.stack([top, (table - top.astype(np.float32)).astype(jnp.bfloat16)])


Y_FORWARD, X_FORWARD, Z_FORWARD, Z_INVERSE, X_INVERSE, Y_INVERSE = map(table_halves, tables())


def dot(a, b, contract=(1, 0)):
    dims = (((contract[0],), (contract[1],)), ((), ()))
    return lax.dot_general(a, b, dims, preferred_element_type=jnp.float32)


def table_times(table_ref, x):
    top, rest = halves(x)
    return dot(table_ref[0], top) + dot(table_ref[1], top) + dot(table_ref[0], rest)


def times_table(x, table_ref):
    top, rest = halves(x)
    return dot(top, table_ref[0]) + dot(rest, table_ref[0]) + dot(top, table_ref[1])


def weights_of(u):
    v = 1.0 - u
    return (
        v * v * v * (1.0 / 6.0),
        (0.5 * u - 1.0) * u * u + (2.0 / 3.0),
        (0.5 * v - 1.0) * v * v + (2.0 / 3.0),
        u * u * u * (1.0 / 6.0),
    )


def slopes_of(u):
    v = 1.0 - u
    return (-0.5 * v * v, (1.5 * u - 2.0) * u, (2.0 - 1.5 * v) * v, 0.5 * u * u)


def pack_kernel(*refs):
    slab = lax.axis_index("slab")
    sources, (mine_ref, other_ref), landed, sem = refs[:6], refs[6:8], refs[8:14], refs[14]
    copies = [
        pltpu.make_async_copy(source, target, sem.at[i])
        for i, (source, target) in enumerate(zip(sources, landed))
    ]
    for copy in copies:
        copy.start()
    for copy in copies:
        copy.wait()
    lambda_ref, a_ref, b_ref, flag_ref, index_ref, weight_ref = landed
    flags = flag_ref[...].astype(jnp.float32)
    steps = flags * (b_ref[...] - a_ref[...])
    core = lax.rem(slab, 2)
    first = (slab - core) * 2
    row = lax.broadcasted_iota(jnp.int32, (WINDOWS, HERE), 0)
    scale = jnp.zeros((WINDOWS, HERE), jnp.float32)
    for w in range(WINDOWS):
        scale = jnp.where(row == w, lambda_ref[w], scale)
    values = [
        index_ref[0].astype(jnp.float32),
        index_ref[1].astype(jnp.float32),
        (index_ref[2] - first).astype(jnp.float32),
    ]
    for axis in range(3):
        values.append(weight_ref[axis, 2] + 2.0 * weight_ref[axis, 3] - weight_ref[axis, 0])
    values += [a_ref[...] + scale * steps, steps]
    for r, value in enumerate(values):
        lower, upper = value[:PAIR], value[PAIR:]
        mine_ref[r] = jnp.where(core == 0, lower, upper)
        other_ref[r] = jnp.where(core == 0, upper, lower)


def places(first, height):
    block = jnp.floor(first * (1.0 / height))
    after = jnp.where(block == float(N // height - 1), 0.0, block + 1.0)
    return block, after, first - height * block


def row_halves(value):
    top = value.astype(jnp.bfloat16).astype(jnp.float32)
    return top, value - top


def wide(row):
    return jnp.broadcast_to(row, (16, LANES)).astype(jnp.bfloat16)


def tall(row):
    return jnp.broadcast_to(row, (8, LANES))


def rows_of(height):
    return lax.broadcasted_iota(jnp.int32, (height, LANES), 0).astype(jnp.float32)


def stencil_tiles(rows, height, start, columns):
    zero = jnp.zeros_like(rows)
    here = [rows == start + jnp.asarray(k, rows.dtype) for k in range(4)]
    past = [rows + jnp.asarray(height, rows.dtype) == start + jnp.asarray(k, rows.dtype) for k in range(1, 4)]
    tiles = []
    for values in columns:
        first = second = zero
        for k in range(4):
            first = jnp.where(here[k], values[k], first)
        for k in range(1, 4):
            second = jnp.where(past[k - 1], values[k], second)
        tiles.append((first, second))
    return tiles


def table_columns(block, after, tiles):
    columns = [[] for _ in tiles]
    zero = jnp.zeros_like(tiles[0][0])
    for b in range(N // 16):
        at, next_at = block == jnp.asarray(b, block.dtype), after == jnp.asarray(b, block.dtype)
        for column, (first, second) in zip(columns, tiles):
            column.append(jnp.where(at, first, jnp.where(next_at, second, zero)))
    return [jnp.concatenate(column, axis=0) for column in columns]


ANY, LOWER, UPPER, BELOW, FAR = range(5)
REACH = {ANY: (0, 4), LOWER: (0, 4), UPPER: (2, 4), BELOW: (0, 3), FAR: (0, 1)}


def plane_parts(kind, plane, parts):
    first, second, third, fourth = parts
    if kind == ANY:
        found = []
        for p in range(DEEP):
            value = 0.0
            for q in range(p + 1):
                value = jnp.where(plane == float(q), parts[p - q], value)
            found.append(value)
        return found
    low = plane < (0.5 if kind in (LOWER, FAR) else 2.5)
    if kind == LOWER:
        return [
            jnp.where(low, first, 0.0),
            jnp.where(low, second, first),
            jnp.where(low, third, second),
            jnp.where(low, fourth, third),
        ]
    if kind == UPPER:
        return [jnp.where(low, first, 0.0), jnp.where(low, second, first)]
    if kind == BELOW:
        return [
            jnp.where(low, third, second),
            jnp.where(low, fourth, third),
            jnp.where(low, 0.0, fourth),
        ]
    return [jnp.where(low, 0.0, fourth)]


def spread_rows(kind, rows, keep):
    block, after, row = places(rows[1], 16)
    keep[0], keep[1], keep[2] = block, after, row
    block, after, row = places(rows[0], 16)
    keep[3], keep[4], keep[5] = block, after, row
    for k, value in enumerate(weights_of(rows[4])):
        keep[6 + k], keep[10 + k] = row_halves(value)
    along_x = weights_of(rows[3])
    for p, depth in enumerate(plane_parts(kind, rows[2], weights_of(rows[5]))):
        for k in range(4):
            top, rest = row_halves(along_x[k] * (rows[6] * depth))
            keep[14 + 8 * p + k], keep[18 + 8 * p + k] = top, rest


def spread_planes(sources, keep, planes):
    for slot, (kind, rows) in enumerate(sources):
        spread_rows(kind, rows, keep.at[slot])
    rows16 = rows_of(16).astype(jnp.bfloat16)
    for w in range(PAIR):
        for slot, (kind, _) in enumerate(sources):
            start, stop = REACH[kind]
            count = stop - start
            left, right = [], []
            for chunk in range(HERE // LANES):
                lanes = slice(chunk * LANES, (chunk + 1) * LANES)
                row = lambda r: wide(keep[slot, r, w : w + 1, lanes])
                four = lambda r: [row(r + k) for k in range(4)]
                tiles = stencil_tiles(rows16, 16, row(2), [four(6), four(10)])
                right.append(jnp.concatenate(table_columns(row(0), row(1), tiles), axis=0))
                tiles = stencil_tiles(
                    rows16, 16, row(5), [four(14 + 4 * i) for i in range(2 * count)]
                )
                found = table_columns(row(3), row(4), tiles)
                left.append(jnp.concatenate(found[0::2] + found[1::2], axis=0))
            both = dot(jnp.concatenate(left, axis=1), jnp.concatenate(right, axis=1), (1, 1))
            height = count * N
            added = both[:height, :N] + both[:height, N:] + both[height:, :N]
            for p in range(count):
                part = added[p * N : p * N + N]
                known = planes[w][start + p]
                planes[w][start + p] = part if known is None else known + part
    return planes


def chip_spread_kernel(own_ref, near_ref, out_ref, influence_ref, keep):
    fill_influence(influence_ref)
    planes = [[None] * DEEP for _ in range(PAIR)]
    here = [(ANY, [ref[r] for r in range(8)]) for ref in (own_ref, near_ref)]
    spread_planes(here, keep, planes)
    for w in range(PAIR):
        for p in range(DEEP):
            out_ref[w, p] = planes[w][p]


def by_core(core, first_ref, second_ref):
    pairs = [(first_ref[r], second_ref[r]) for r in range(8)]
    return (
        [jnp.where(core == 0, a, b) for a, b in pairs],
        [jnp.where(core == 0, b, a) for a, b in pairs],
    )


def spread_kernel(
    chip_ref, same_ref, cross_ref, y_hbm, x_hbm, out_ref, keep, y_ref, x_ref, sem
):
    copies = [
        pltpu.make_async_copy(y_hbm, y_ref, sem.at[0]),
        pltpu.make_async_copy(x_hbm, x_ref, sem.at[1]),
    ]
    for copy in copies:
        copy.start()
    core = lax.rem(lax.axis_index("slab"), 2)
    far, below = by_core(core, same_ref, cross_ref)
    planes = [[chip_ref[w, p] for p in range(DEEP)] for w in range(PAIR)]
    spread_planes([(BELOW, below), (FAR, far)], keep, planes)
    for copy in copies:
        copy.wait()
    for first in range(0, DEEP, 2):
        stacked = jnp.concatenate(
            [jnp.concatenate([planes[0][p], planes[1][p]], axis=1) for p in (first, first + 1)],
            axis=0,
        )
        turned = times_table(stacked, y_ref)
        upright = jnp.concatenate(
            [
                jnp.concatenate([turned[b : b + N, :N], turned[b : b + N, N:]], axis=0)
                for b in (0, N)
            ],
            axis=1,
        )
        columns = table_times(x_ref, upright)
        for b in range(2):
            out_ref[:, first + b] = columns[:, b * N : b * N + N].reshape(N // 4, 8, N)


def frequency(counter):
    return jnp.where(counter >= N // 2, counter - N, counter).astype(jnp.float32) / N


def fill_influence(out_ref):
    slab = lax.axis_index("slab")
    first = (slab - lax.rem(slab, 2)) * 2
    shape = (N, N)
    freq_z = frequency(lax.broadcasted_iota(jnp.int32, shape, 0))
    freq_y = frequency(lax.broadcasted_iota(jnp.int32, shape, 1))
    flat = freq_z * freq_z + freq_y * freq_y
    for j in range(4):
        freq_x = frequency(jnp.full(shape, first + j, jnp.int32))
        squared = flat + freq_x * freq_x
        positive = squared > 0
        safe = jnp.where(positive, squared, 1.0)
        out_ref[:, j * N : j * N + N] = jnp.where(
            positive, jnp.exp(-gauss_width * squared) / (math.pi * N * N * N * safe), 0.0
        )


def column_kernel(in_ref, influence_ref, forward_ref, inverse_ref, out_ref):
    part = lambda r: in_ref[pl.ds(r, N, stride=8), :]
    columns = jnp.concatenate(
        [jnp.concatenate([part(j), part(4 + j)], axis=0) for j in range(4)], axis=1
    )
    depth = table_times(forward_ref, columns)
    influence = influence_ref[...]
    depth = jnp.concatenate([depth[:N] * influence, depth[N:] * influence], axis=0)
    back = table_times(inverse_ref, depth)
    for j in range(4):
        out_ref[pl.ds(j, N, stride=8), :] = back[:N, j * N : j * N + N]
        out_ref[pl.ds(4 + j, N, stride=8), :] = back[N:, j * N : j * N + N]


def sample_rows(kind, rows, keep):
    block, after, row = places(rows[1], 16)
    keep[0], keep[1], keep[2] = block, after, row
    for k, value in enumerate(weights_of(rows[4])):
        keep[3 + k], keep[7 + k] = row_halves(value)
    for k, value in enumerate(slopes_of(rows[4])):
        keep[11 + k], keep[15 + k] = row_halves(value)
    block, after, row = places(rows[0], 8)
    keep[19], keep[20], keep[21] = block, after, row
    for k, (value, slope) in enumerate(zip(weights_of(rows[3]), slopes_of(rows[3]))):
        keep[22 + k], keep[26 + k] = value, slope
    for p, depth in enumerate(plane_parts(kind, rows[2], weights_of(rows[5]))):
        keep[30 + p] = depth
    for p, steep in enumerate(plane_parts(kind, rows[2], slopes_of(rows[5]))):
        keep[34 + p] = steep
    keep[38], keep[39] = rows[6], rows[7]


def sample_kernel(
    in_ref,
    own_ref,
    near_ref,
    same_ref,
    cross_ref,
    x_ref,
    y_ref,
    own_out,
    near_out,
    same_out,
    cross_out,
    sum_out,
    keep,
    forces,
    sums,
):
    core = lax.rem(lax.axis_index("slab"), 2)
    pairs = []
    for first in range(0, DEEP, 2):
        columns = jnp.concatenate(
            [in_ref[:, b].reshape(2 * N, N) for b in (first, first + 1)], axis=1
        )
        upright = table_times(x_ref, columns)
        flat = jnp.concatenate(
            [
                jnp.concatenate([upright[:N, b : b + N], upright[N:, b : b + N]], axis=1)
                for b in (0, N)
            ],
            axis=0,
        )
        pairs.append(times_table(flat, y_ref))
    pairs = jnp.concatenate(pairs, axis=0)
    lower, upper = by_core(core, own_ref, near_ref)
    far, below = by_core(core, same_ref, cross_ref)
    sources = ((LOWER, lower), (UPPER, upper), (BELOW, below), (FAR, far))
    for slot, (kind, rows) in enumerate(sources):
        sample_rows(kind, rows, keep.at[slot])
    rows16 = rows_of(16).astype(jnp.bfloat16)
    rows8 = rows_of(8)
    for w in range(PAIR):
        planes = jnp.concatenate(halves(pairs[:, w * N : w * N + N]), axis=1)
        energy = jnp.zeros((1, LANES), jnp.float32)
        slope = jnp.zeros((1, LANES), jnp.float32)
        for slot, (kind, _) in enumerate(sources):
            start, stop = REACH[kind]
            count = stop - start
            tops, rests = [], []
            for chunk in range(HERE // LANES):
                lanes = slice(chunk * LANES, (chunk + 1) * LANES)
                row = lambda r: wide(keep[slot, r, w : w + 1, lanes])
                four = lambda r: [row(r + k) for k in range(4)]
                tiles = stencil_tiles(rows16, 16, row(2), [four(3 + 4 * i) for i in range(4)])
                found = table_columns(row(0), row(1), tiles)
                tops.append(jnp.concatenate([found[0], found[2]], axis=1))
                rests.append(jnp.concatenate([found[1], found[3]], axis=1))
            tops = jnp.concatenate(tops, axis=1)
            rests = jnp.concatenate(rests, axis=1)
            used = planes[start * N : stop * N]
            levels = dot(used, jnp.concatenate([tops, tops], axis=0)) + dot(used[:, :N], rests)
            for chunk in range(HERE // LANES):
                lanes = slice(chunk * LANES, (chunk + 1) * LANES)
                row = lambda r: tall(keep[slot, r, w : w + 1, lanes])
                four = lambda r: [row(r + k) for k in range(4)]
                block, after = row(19), row(20)
                tiles = stencil_tiles(rows8, 8, row(21), [four(22), four(26)])
                near = [[None] * 2 for _ in range(2 * count)]
                for b in range(N // 8):
                    at, next_at = block == float(b), after == float(b)
                    for q in range(2 * count):
                        p, slant = q // 2, q % 2
                        level = levels[
                            p * N + b * 8 : p * N + b * 8 + 8,
                            (2 * chunk + slant) * LANES : (2 * chunk + slant + 1) * LANES,
                        ]
                        if b == 0:
                            near[q] = [level, level]
                        else:
                            near[q][0] = jnp.where(at, level, near[q][0])
                            near[q][1] = jnp.where(next_at, level, near[q][1])
                total = [jnp.zeros((8, LANES), jnp.float32) for _ in range(4)]
                for half in range(2):
                    along, along_dx = tiles[0][half], tiles[1][half]
                    plain = near[0][half] * row(30)
                    over_z = near[0][half] * row(34)
                    over_y = near[1][half] * row(30)
                    for p in range(1, count):
                        plain = plain + near[2 * p][half] * row(30 + p)
                        over_z = over_z + near[2 * p][half] * row(34 + p)
                        over_y = over_y + near[2 * p + 1][half] * row(30 + p)
                    total[0] = total[0] + along * plain
                    total[1] = total[1] + along_dx * plain
                    total[2] = total[2] + along * over_y
                    total[3] = total[3] + along * over_z
                total = [jnp.sum(t, axis=0, keepdims=True) for t in total]
                charge = keep[slot, 38, w : w + 1, lanes]
                for d in range(3):
                    forces[slot, d, w : w + 1, lanes] = -charge * total[1 + d]
                energy = energy + charge * total[0]
                slope = slope + keep[slot, 39, w : w + 1, lanes] * total[0]
        sums[w : w + 1, :] = energy
        sums[PAIR + w : PAIR + w + 1, :] = slope
    own_out[...] = jnp.where(core == 0, forces[0], forces[1])
    near_out[...] = jnp.where(core == 0, forces[1], forces[0])
    same_out[...] = jnp.where(core == 0, forces[3], forces[2])
    cross_out[...] = jnp.where(core == 0, forces[2], forces[3])
    added = jnp.sum(sums[...], axis=1, keepdims=True)
    shape = (2 * PAIR, LANES)
    row = lax.broadcasted_iota(jnp.int32, shape, 0)
    place = PAIR * core + jnp.where(row < PAIR, row, row - PAIR + WINDOWS)
    here = lax.broadcasted_iota(jnp.int32, shape, 1) == place
    line = jnp.sum(jnp.where(here, added, 0.0), axis=0, keepdims=True)
    sum_out[...] = jnp.broadcast_to(line, (SLABS, LANES))


def finish_kernel(
    own_ref, near_ref, same_ref, cross_ref, sum_ref, force_out, energy_out, slope_out
):
    core = lax.rem(lax.axis_index("slab"), 2)
    mine = own_ref[...] + same_ref[...]
    other = near_ref[...] + cross_ref[...]
    force_out[:, :PAIR] = jnp.where(core == 0, mine, other)
    force_out[:, PAIR:] = jnp.where(core == 0, other, mine)
    line = jnp.sum(sum_ref[...], axis=0, keepdims=True)
    lane = lax.broadcasted_iota(jnp.int32, (1, LANES), 1)
    for w in range(WINDOWS):
        energy_out[w] = jnp.sum(jnp.where(lane == w, line, 0.0)) * (0.5 / ATOMS)
        slope_out[w] = jnp.sum(jnp.where(lane == WINDOWS + w, line, 0.0)) * (1.0 / ATOMS)


in_vmem = pl.BlockSpec(memory_space=pltpu.VMEM)
in_smem = pl.BlockSpec(memory_space=pltpu.SMEM)
in_hbm = pl.BlockSpec(memory_space=pltpu.HBM)
table_scratch = pltpu.VMEM((2, 2 * N, 2 * N), jnp.bfloat16)


def far_away(array):
    return pltpu.with_memory_space_constraint(array, pltpu.HBM)


def f32(*shape):
    return jax.ShapeDtypeStruct(shape, jnp.float32)


def run(kernel, out_shape, in_specs, operands, scratch=(), mib=16):
    several = isinstance(out_shape, tuple)
    return pl.pallas_call(
        kernel,
        out_shape=out_shape,
        in_specs=in_specs,
        out_specs=(in_vmem,) * len(out_shape) if several else in_vmem,
        scratch_shapes=list(scratch),
        compiler_params=pltpu.CompilerParams(vmem_limit_bytes=mib << 20),
        name=kernel.__name__,
    )(*operands)


def moved(value, pairs, back=False):
    return lax.ppermute(value, "slab", [pair[::-1] if back else pair for pair in pairs])


TO_PARTNER = [(d, d ^ 1) for d in range(SLABS)]
UP_SAME = [(d, (d + 2) % SLABS) for d in range(SLABS)]
UP_CROSS = [(d, ((d ^ 1) + 2) % SLABS) for d in range(SLABS)]
CORES = [list(range(c, SLABS, 2)) for c in range(2)]


def exchanged(value):
    return lax.all_to_all(value, "slab", 0, 0, tiled=True, axis_index_groups=CORES)


def body(lambdas, charge_a, charge_b, perturbed, grid_index, spline_weights, spline_slopes):
    inputs = tuple(
        far_away(a)
        for a in (lambdas, charge_a, charge_b, perturbed, grid_index, spline_weights)
    )
    atoms = f32(8, PAIR, HERE)
    own, other = run(
        pack_kernel,
        (atoms, atoms),
        [in_hbm] * 6,
        inputs,
        [pltpu.SMEM((WINDOWS,), jnp.float32)]
        + [pltpu.VMEM(a.shape, a.dtype) for a in inputs[1:]]
        + [pltpu.SemaphoreType.DMA((6,))],
        mib=4,
    )
    near = moved(other, TO_PARTNER)
    same = moved(own, UP_SAME)
    cross = moved(other, UP_CROSS)
    kept = lambda count, rows: pltpu.VMEM((count, rows, PAIR, HERE), jnp.float32)
    from_chip, influence = run(
        chip_spread_kernel,
        (f32(PAIR, DEEP, N, N), f32(N, 4 * N)),
        [in_vmem] * 2,
        (own, near),
        [kept(2, 46)],
    )
    spectrum = run(
        spread_kernel,
        f32(CHIPS, DEEP, 8, N),
        [in_vmem] * 3 + [in_hbm] * 2,
        (
            from_chip,
            same,
            cross,
            far_away(jnp.asarray(Y_FORWARD)),
            far_away(jnp.asarray(X_FORWARD)),
        ),
        [kept(2, 46), table_scratch, table_scratch, pltpu.SemaphoreType.DMA((2,))],
    )
    columns = exchanged(spectrum.reshape(CHIPS, 8 * DEEP, N))
    columns = run(
        column_kernel,
        f32(8 * N, N),
        [in_vmem] * 4,
        (columns.reshape(8 * N, N), influence, Z_FORWARD, Z_INVERSE),
        mib=8,
    )
    levels = exchanged(columns.reshape(CHIPS, 8 * DEEP, N))
    part = f32(3, PAIR, HERE)
    mine, for_near, for_same, for_cross, sums = run(
        sample_kernel,
        (part, part, part, part, f32(SLABS, N)),
        [in_vmem] * 7,
        (levels.reshape(CHIPS, DEEP, 8, N), own, near, same, cross, X_INVERSE, Y_INVERSE),
        [
            kept(4, 40),
            pltpu.VMEM((4, 3, PAIR, HERE), jnp.float32),
            pltpu.VMEM((2 * PAIR, LANES), jnp.float32),
        ],
    )
    from_near = moved(for_near, TO_PARTNER, back=True)
    from_same = moved(for_same, UP_SAME, back=True)
    from_cross = moved(for_cross, UP_CROSS, back=True)
    sums = lax.all_to_all(sums.reshape(SLABS, 1, N), "slab", 0, 0, tiled=True)
    return pl.pallas_call(
        finish_kernel,
        out_shape=(f32(3, WINDOWS, HERE), f32(WINDOWS), f32(WINDOWS)),
        in_specs=[in_vmem] * 5,
        out_specs=(in_vmem, in_smem, in_smem),
        compiler_params=pltpu.CompilerParams(vmem_limit_bytes=4 << 20),
        name="finish_kernel",
    )(mine, from_near, from_same, from_cross, sums.reshape(SLABS, N))


def solution(mesh):
    return jax.shard_map(
        body,
        mesh=mesh,
        in_specs=(
            P("win"),
            P("win", "slab"),
            P("win", "slab"),
            P("win", "slab"),
            P(None, "win", "slab"),
            P(None, None, "win", "slab"),
            P(None, None, "win", "slab"),
        ),
        out_specs=(P(None, "win", "slab"), P("win"), P("win")),
        check_vma=False,
    )
```

```python
import math

import jax
import jax.numpy as jnp
import numpy as np
from jax import lax
from jax.experimental import pallas as pl
from jax.experimental.pallas import tpu as pltpu
from jax.sharding import PartitionSpec as P

N = 128
LANES = 128
WINDOWS = 4
HERE = 512
SLABS = 64
CHIPS = SLABS // 2
PAIR = WINDOWS // 2
DEEP = 4
ATOMS = SLABS * HERE
gauss_width = 2.0


def blocks(real, imaginary):
    return np.block([[real, -imaginary], [imaginary, real]])


def tables():
    k = np.arange(N)
    angle = 2.0 * np.pi * ((k[:, None] * k[None, :]) % N) / N
    cosine, sine = np.cos(angle), np.sin(angle)
    forward = blocks(cosine, -sine)
    inverse = blocks(cosine, sine)
    order = np.arange(2 * N).reshape(2, N // 4, 4).transpose(1, 0, 2).ravel()
    return tuple(
        np.ascontiguousarray(m, dtype=np.float32)
        for m in (
            forward.T,
            forward[order],
            forward,
            inverse,
            inverse[:, order],
            inverse.T,
        )
    )


def halves(x):
    top = x.astype(jnp.bfloat16)
    return top, (x - top.astype(jnp.float32)).astype(jnp.bfloat16)


def table_halves(table):
    top = table.astype(jnp.bfloat16)
    return np.stack([top, (table - top.astype(np.float32)).astype(jnp.bfloat16)])


Y_FORWARD, X_FORWARD, Z_FORWARD, Z_INVERSE, X_INVERSE, Y_INVERSE = map(table_halves, tables())


def dot(a, b, contract=(1, 0)):
    dims = (((contract[0],), (contract[1],)), ((), ()))
    return lax.dot_general(a, b, dims, preferred_element_type=jnp.float32)


def table_times(table_ref, x):
    top, rest = halves(x)
    return dot(table_ref[0], top) + dot(table_ref[1], top) + dot(table_ref[0], rest)


def times_table(x, table_ref):
    top, rest = halves(x)
    return dot(top, table_ref[0]) + dot(rest, table_ref[0]) + dot(top, table_ref[1])


def weights_of(u):
    v = 1.0 - u
    return (
        v * v * v * (1.0 / 6.0),
        (0.5 * u - 1.0) * u * u + (2.0 / 3.0),
        (0.5 * v - 1.0) * v * v + (2.0 / 3.0),
        u * u * u * (1.0 / 6.0),
    )


def slopes_of(u):
    v = 1.0 - u
    return (-0.5 * v * v, (1.5 * u - 2.0) * u, (2.0 - 1.5 * v) * v, 0.5 * u * u)


def pack_kernel(*refs):
    slab = lax.axis_index("slab")
    sources, (mine_ref, other_ref), landed, sem = refs[:6], refs[6:8], refs[8:14], refs[14]
    copies = [
        pltpu.make_async_copy(source, target, sem.at[i])
        for i, (source, target) in enumerate(zip(sources, landed))
    ]
    for copy in copies:
        copy.start()
    for copy in copies:
        copy.wait()
    lambda_ref, a_ref, b_ref, flag_ref, index_ref, weight_ref = landed
    flags = flag_ref[...].astype(jnp.float32)
    steps = flags * (b_ref[...] - a_ref[...])
    core = lax.rem(slab, 2)
    first = (slab - core) * 2
    row = lax.broadcasted_iota(jnp.int32, (WINDOWS, HERE), 0)
    scale = jnp.zeros((WINDOWS, HERE), jnp.float32)
    for w in range(WINDOWS):
        scale = jnp.where(row == w, lambda_ref[w], scale)
    values = [
        index_ref[0].astype(jnp.float32),
        index_ref[1].astype(jnp.float32),
        (index_ref[2] - first).astype(jnp.float32),
    ]
    for axis in range(3):
        values.append(weight_ref[axis, 2] + 2.0 * weight_ref[axis, 3] - weight_ref[axis, 0])
    values += [a_ref[...] + scale * steps, steps]
    for r, value in enumerate(values):
        lower, upper = value[:PAIR], value[PAIR:]
        mine_ref[r] = jnp.where(core == 0, lower, upper)
        other_ref[r] = jnp.where(core == 0, upper, lower)


def places(first, height):
    block = jnp.floor(first * (1.0 / height))
    after = jnp.where(block == float(N // height - 1), 0.0, block + 1.0)
    return block, after, first - height * block


def row_halves(value):
    top = value.astype(jnp.bfloat16).astype(jnp.float32)
    return top, value - top


def wide(row):
    return jnp.broadcast_to(row, (16, LANES)).astype(jnp.bfloat16)


def tall(row):
    return jnp.broadcast_to(row, (8, LANES))


def rows_of(height):
    return lax.broadcasted_iota(jnp.int32, (height, LANES), 0).astype(jnp.float32)


def stencil_tiles(rows, height, start, columns):
    zero = jnp.zeros_like(rows)
    here = [rows == start + jnp.asarray(k, rows.dtype) for k in range(4)]
    past = [rows + jnp.asarray(height, rows.dtype) == start + jnp.asarray(k, rows.dtype) for k in range(1, 4)]
    tiles = []
    for values in columns:
        first = second = zero
        for k in range(4):
            first = jnp.where(here[k], values[k], first)
        for k in range(1, 4):
            second = jnp.where(past[k - 1], values[k], second)
        tiles.append((first, second))
    return tiles


def table_columns(block, after, tiles):
    columns = [[] for _ in tiles]
    zero = jnp.zeros_like(tiles[0][0])
    for b in range(N // 16):
        at, next_at = block == jnp.asarray(b, block.dtype), after == jnp.asarray(b, block.dtype)
        for column, (first, second) in zip(columns, tiles):
            column.append(jnp.where(at, first, jnp.where(next_at, second, zero)))
    return [jnp.concatenate(column, axis=0) for column in columns]


ANY, LOWER, UPPER, BELOW, FAR = range(5)
REACH = {ANY: (0, 4), LOWER: (0, 4), UPPER: (2, 4), BELOW: (0, 3), FAR: (0, 1)}


def plane_parts(kind, plane, parts):
    first, second, third, fourth = parts
    if kind == ANY:
        found = []
        for p in range(DEEP):
            value = 0.0
            for q in range(p + 1):
                value = jnp.where(plane == float(q), parts[p - q], value)
            found.append(value)
        return found
    low = plane < (0.5 if kind in (LOWER, FAR) else 2.5)
    if kind == LOWER:
        return [
            jnp.where(low, first, 0.0),
            jnp.where(low, second, first),
            jnp.where(low, third, second),
            jnp.where(low, fourth, third),
        ]
    if kind == UPPER:
        return [jnp.where(low, first, 0.0), jnp.where(low, second, first)]
    if kind == BELOW:
        return [
            jnp.where(low, third, second),
            jnp.where(low, fourth, third),
            jnp.where(low, 0.0, fourth),
        ]
    return [jnp.where(low, 0.0, fourth)]


def spread_rows(kind, rows, keep):
    block, after, row = places(rows[1], 16)
    keep[0], keep[1], keep[2] = block, after, row
    block, after, row = places(rows[0], 16)
    keep[3], keep[4], keep[5] = block, after, row
    for k, value in enumerate(weights_of(rows[4])):
        keep[6 + k], keep[10 + k] = row_halves(value)
    along_x = weights_of(rows[3])
    for p, depth in enumerate(plane_parts(kind, rows[2], weights_of(rows[5]))):
        for k in range(4):
            top, rest = row_halves(along_x[k] * (rows[6] * depth))
            keep[14 + 8 * p + k], keep[18 + 8 * p + k] = top, rest


def spread_planes(sources, keep, planes):
    for slot, (kind, rows) in enumerate(sources):
        spread_rows(kind, rows, keep.at[slot])
    rows16 = rows_of(16).astype(jnp.bfloat16)
    for w in range(PAIR):
        for slot, (kind, _) in enumerate(sources):
            start, stop = REACH[kind]
            count = stop - start
            left, right = [], []
            for chunk in range(HERE // LANES):
                lanes = slice(chunk * LANES, (chunk + 1) * LANES)
                row = lambda r: wide(keep[slot, r, w : w + 1, lanes])
                four = lambda r: [row(r + k) for k in range(4)]
                tiles = stencil_tiles(rows16, 16, row(2), [four(6), four(10)])
                right.append(jnp.concatenate(table_columns(row(0), row(1), tiles), axis=0))
                tiles = stencil_tiles(
                    rows16, 16, row(5), [four(14 + 4 * i) for i in range(2 * count)]
                )
                found = table_columns(row(3), row(4), tiles)
                left.append(jnp.concatenate(found[0::2] + found[1::2], axis=0))
            both = dot(jnp.concatenate(left, axis=1), jnp.concatenate(right, axis=1), (1, 1))
            height = count * N
            added = both[:height, :N] + both[:height, N:] + both[height:, :N]
            for p in range(count):
                part = added[p * N : p * N + N]
                known = planes[w][start + p]
                planes[w][start + p] = part if known is None else known + part
    return planes


def chip_spread_kernel(own_ref, near_ref, out_ref, influence_ref, keep):
    fill_influence(influence_ref)
    planes = [[None] * DEEP for _ in range(PAIR)]
    here = [(ANY, [ref[r] for r in range(8)]) for ref in (own_ref, near_ref)]
    spread_planes(here, keep, planes)
    for w in range(PAIR):
        for p in range(DEEP):
            out_ref[w, p] = planes[w][p]


def by_core(core, first_ref, second_ref):
    pairs = [(first_ref[r], second_ref[r]) for r in range(8)]
    return (
        [jnp.where(core == 0, a, b) for a, b in pairs],
        [jnp.where(core == 0, b, a) for a, b in pairs],
    )


def spread_kernel(
    chip_ref, same_ref, cross_ref, y_hbm, x_hbm, out_ref, keep, y_ref, x_ref, sem
):
    copies = [
        pltpu.make_async_copy(y_hbm, y_ref, sem.at[0]),
        pltpu.make_async_copy(x_hbm, x_ref, sem.at[1]),
    ]
    for copy in copies:
        copy.start()
    core = lax.rem(lax.axis_index("slab"), 2)
    far, below = by_core(core, same_ref, cross_ref)
    planes = [[chip_ref[w, p] for p in range(DEEP)] for w in range(PAIR)]
    spread_planes([(BELOW, below), (FAR, far)], keep, planes)
    for copy in copies:
        copy.wait()
    for first in range(0, DEEP, 2):
        stacked = jnp.concatenate(
            [jnp.concatenate([planes[0][p], planes[1][p]], axis=1) for p in (first, first + 1)],
            axis=0,
        )
        turned = times_table(stacked, y_ref)
        upright = jnp.concatenate(
            [
                jnp.concatenate([turned[b : b + N, :N], turned[b : b + N, N:]], axis=0)
                for b in (0, N)
            ],
            axis=1,
        )
        columns = table_times(x_ref, upright)
        for b in range(2):
            out_ref[:, first + b] = columns[:, b * N : b * N + N].reshape(N // 4, 8, N)


def frequency(counter):
    return jnp.where(counter >= N // 2, counter - N, counter).astype(jnp.float32) / N


def fill_influence(out_ref):
    slab = lax.axis_index("slab")
    first = (slab - lax.rem(slab, 2)) * 2
    shape = (N, N)
    freq_z = frequency(lax.broadcasted_iota(jnp.int32, shape, 0))
    freq_y = frequency(lax.broadcasted_iota(jnp.int32, shape, 1))
    flat = freq_z * freq_z + freq_y * freq_y
    for j in range(4):
        freq_x = frequency(jnp.full(shape, first + j, jnp.int32))
        squared = flat + freq_x * freq_x
        positive = squared > 0
        safe = jnp.where(positive, squared, 1.0)
        out_ref[:, j * N : j * N + N] = jnp.where(
            positive, jnp.exp(-gauss_width * squared) / (math.pi * N * N * N * safe), 0.0
        )


def column_kernel(in_ref, influence_ref, forward_ref, inverse_ref, out_ref):
    part = lambda r: in_ref[pl.ds(r, N, stride=8), :]
    columns = jnp.concatenate(
        [jnp.concatenate([part(j), part(4 + j)], axis=0) for j in range(4)], axis=1
    )
    depth = table_times(forward_ref, columns)
    influence = influence_ref[...]
    depth = jnp.concatenate([depth[:N] * influence, depth[N:] * influence], axis=0)
    back = table_times(inverse_ref, depth)
    for j in range(4):
        out_ref[pl.ds(j, N, stride=8), :] = back[:N, j * N : j * N + N]
        out_ref[pl.ds(4 + j, N, stride=8), :] = back[N:, j * N : j * N + N]


def sample_rows(kind, rows, keep):
    block, after, row = places(rows[1], 16)
    keep[0], keep[1], keep[2] = block, after, row
    for k, value in enumerate(weights_of(rows[4])):
        keep[3 + k], keep[7 + k] = row_halves(value)
    for k, value in enumerate(slopes_of(rows[4])):
        keep[11 + k], keep[15 + k] = row_halves(value)
    block, after, row = places(rows[0], 8)
    keep[19], keep[20], keep[21] = block, after, row
    for k, (value, slope) in enumerate(zip(weights_of(rows[3]), slopes_of(rows[3]))):
        keep[22 + k], keep[26 + k] = value, slope
    for p, depth in enumerate(plane_parts(kind, rows[2], weights_of(rows[5]))):
        keep[30 + p] = depth
    for p, steep in enumerate(plane_parts(kind, rows[2], slopes_of(rows[5]))):
        keep[34 + p] = steep
    keep[38], keep[39] = rows[6], rows[7]


def sample_kernel(
    in_ref,
    own_ref,
    near_ref,
    same_ref,
    cross_ref,
    x_ref,
    y_ref,
    own_out,
    near_out,
    same_out,
    cross_out,
    sum_out,
    keep,
    forces,
    sums,
):
    core = lax.rem(lax.axis_index("slab"), 2)
    pairs = []
    for first in range(0, DEEP, 2):
        columns = jnp.concatenate(
            [in_ref[:, b].reshape(2 * N, N) for b in (first, first + 1)], axis=1
        )
        upright = table_times(x_ref, columns)
        flat = jnp.concatenate(
            [
                jnp.concatenate([upright[:N, b : b + N], upright[N:, b : b + N]], axis=1)
                for b in (0, N)
            ],
            axis=0,
        )
        pairs.append(times_table(flat, y_ref))
    pairs = jnp.concatenate(pairs, axis=0)
    lower, upper = by_core(core, own_ref, near_ref)
    far, below = by_core(core, same_ref, cross_ref)
    sources = ((LOWER, lower), (UPPER, upper), (BELOW, below), (FAR, far))
    for slot, (kind, rows) in enumerate(sources):
        sample_rows(kind, rows, keep.at[slot])
    rows16 = rows_of(16).astype(jnp.bfloat16)
    rows8 = rows_of(8)
    for w in range(PAIR):
        planes = jnp.concatenate(halves(pairs[:, w * N : w * N + N]), axis=1)
        energy = jnp.zeros((1, LANES), jnp.float32)
        slope = jnp.zeros((1, LANES), jnp.float32)
        for slot, (kind, _) in enumerate(sources):
            start, stop = REACH[kind]
            count = stop - start
            tops, rests = [], []
            for chunk in range(HERE // LANES):
                lanes = slice(chunk * LANES, (chunk + 1) * LANES)
                row = lambda r: wide(keep[slot, r, w : w + 1, lanes])
                four = lambda r: [row(r + k) for k in range(4)]
                tiles = stencil_tiles(rows16, 16, row(2), [four(3 + 4 * i) for i in range(4)])
                found = table_columns(row(0), row(1), tiles)
                tops.append(jnp.concatenate([found[0], found[2]], axis=1))
                rests.append(jnp.concatenate([found[1], found[3]], axis=1))
            tops = jnp.concatenate(tops, axis=1)
            rests = jnp.concatenate(rests, axis=1)
            used = planes[start * N : stop * N]
            levels = dot(used, jnp.concatenate([tops, tops], axis=0)) + dot(used[:, :N], rests)
            for chunk in range(HERE // LANES):
                lanes = slice(chunk * LANES, (chunk + 1) * LANES)
                row = lambda r: tall(keep[slot, r, w : w + 1, lanes])
                four = lambda r: [row(r + k) for k in range(4)]
                block, after = row(19), row(20)
                tiles = stencil_tiles(rows8, 8, row(21), [four(22), four(26)])
                near = [[None] * 2 for _ in range(2 * count)]
                for b in range(N // 8):
                    at, next_at = block == float(b), after == float(b)
                    for q in range(2 * count):
                        p, slant = q // 2, q % 2
                        level = levels[
                            p * N + b * 8 : p * N + b * 8 + 8,
                            (2 * chunk + slant) * LANES : (2 * chunk + slant + 1) * LANES,
                        ]
                        if b == 0:
                            near[q] = [level, level]
                        else:
                            near[q][0] = jnp.where(at, level, near[q][0])
                            near[q][1] = jnp.where(next_at, level, near[q][1])
                total = [jnp.zeros((8, LANES), jnp.float32) for _ in range(4)]
                for half in range(2):
                    along, along_dx = tiles[0][half], tiles[1][half]
                    plain = near[0][half] * row(30)
                    over_z = near[0][half] * row(34)
                    over_y = near[1][half] * row(30)
                    for p in range(1, count):
                        plain = plain + near[2 * p][half] * row(30 + p)
                        over_z = over_z + near[2 * p][half] * row(34 + p)
                        over_y = over_y + near[2 * p + 1][half] * row(30 + p)
                    total[0] = total[0] + along * plain
                    total[1] = total[1] + along_dx * plain
                    total[2] = total[2] + along * over_y
                    total[3] = total[3] + along * over_z
                total = [jnp.sum(t, axis=0, keepdims=True) for t in total]
                charge = keep[slot, 38, w : w + 1, lanes]
                for d in range(3):
                    forces[slot, d, w : w + 1, lanes] = -charge * total[1 + d]
                energy = energy + charge * total[0]
                slope = slope + keep[slot, 39, w : w + 1, lanes] * total[0]
        sums[w : w + 1, :] = energy
        sums[PAIR + w : PAIR + w + 1, :] = slope
    own_out[...] = jnp.where(core == 0, forces[0], forces[1])
    near_out[...] = jnp.where(core == 0, forces[1], forces[0])
    same_out[...] = jnp.where(core == 0, forces[3], forces[2])
    cross_out[...] = jnp.where(core == 0, forces[2], forces[3])
    added = jnp.sum(sums[...], axis=1, keepdims=True)
    shape = (2 * PAIR, LANES)
    row = lax.broadcasted_iota(jnp.int32, shape, 0)
    place = PAIR * core + jnp.where(row < PAIR, row, row - PAIR + WINDOWS)
    here = lax.broadcasted_iota(jnp.int32, shape, 1) == place
    line = jnp.sum(jnp.where(here, added, 0.0), axis=0, keepdims=True)
    sum_out[...] = jnp.broadcast_to(line, (SLABS, LANES))


def finish_kernel(
    own_ref, near_ref, same_ref, cross_ref, sum_ref, force_out, energy_out, slope_out
):
    core = lax.rem(lax.axis_index("slab"), 2)
    mine = own_ref[...] + same_ref[...]
    other = near_ref[...] + cross_ref[...]
    force_out[:, :PAIR] = jnp.where(core == 0, mine, other)
    force_out[:, PAIR:] = jnp.where(core == 0, other, mine)
    line = jnp.sum(sum_ref[...], axis=0, keepdims=True)
    lane = lax.broadcasted_iota(jnp.int32, (1, LANES), 1)
    for w in range(WINDOWS):
        energy_out[w] = jnp.sum(jnp.where(lane == w, line, 0.0)) * (0.5 / ATOMS)
        slope_out[w] = jnp.sum(jnp.where(lane == WINDOWS + w, line, 0.0)) * (1.0 / ATOMS)


in_vmem = pl.BlockSpec(memory_space=pltpu.VMEM)
in_smem = pl.BlockSpec(memory_space=pltpu.SMEM)
in_hbm = pl.BlockSpec(memory_space=pltpu.HBM)
table_scratch = pltpu.VMEM((2, 2 * N, 2 * N), jnp.bfloat16)


def far_away(array):
    return pltpu.with_memory_space_constraint(array, pltpu.HBM)


def f32(*shape):
    return jax.ShapeDtypeStruct(shape, jnp.float32)


def run(kernel, out_shape, in_specs, operands, scratch=(), mib=16, flags=None):
    several = isinstance(out_shape, tuple)
    return pl.pallas_call(
        kernel,
        out_shape=out_shape,
        in_specs=in_specs,
        out_specs=(in_vmem,) * len(out_shape) if several else in_vmem,
        scratch_shapes=list(scratch),
        compiler_params=pltpu.CompilerParams(vmem_limit_bytes=mib << 20, flags=flags),
        name=kernel.__name__,
    )(*operands)


def moved(value, pairs, back=False):
    return lax.ppermute(value, "slab", [pair[::-1] if back else pair for pair in pairs])


TO_PARTNER = [(d, d ^ 1) for d in range(SLABS)]
UP_SAME = [(d, (d + 2) % SLABS) for d in range(SLABS)]
UP_CROSS = [(d, ((d ^ 1) + 2) % SLABS) for d in range(SLABS)]
CORES = [list(range(c, SLABS, 2)) for c in range(2)]


def exchanged(value):
    return lax.all_to_all(value, "slab", 0, 0, tiled=True, axis_index_groups=CORES)


def body(lambdas, charge_a, charge_b, perturbed, grid_index, spline_weights, spline_slopes):
    inputs = tuple(
        far_away(a)
        for a in (lambdas, charge_a, charge_b, perturbed, grid_index, spline_weights)
    )
    atoms = f32(8, PAIR, HERE)
    own, other = run(
        pack_kernel,
        (atoms, atoms),
        [in_hbm] * 6,
        inputs,
        [pltpu.SMEM((WINDOWS,), jnp.float32)]
        + [pltpu.VMEM(a.shape, a.dtype) for a in inputs[1:]]
        + [pltpu.SemaphoreType.DMA((6,))],
        mib=4,
    )
    near = moved(other, TO_PARTNER)
    same = moved(own, UP_SAME)
    cross = moved(other, UP_CROSS)
    kept = lambda count, rows: pltpu.VMEM((count, rows, PAIR, HERE), jnp.float32)
    from_chip, influence = run(
        chip_spread_kernel,
        (f32(PAIR, DEEP, N, N), f32(N, 4 * N)),
        [in_vmem] * 2,
        (own, near),
        [kept(2, 46)],
    )
    spectrum = run(
        spread_kernel,
        f32(CHIPS, DEEP, 8, N),
        [in_vmem] * 3 + [in_hbm] * 2,
        (
            from_chip,
            same,
            cross,
            far_away(jnp.asarray(Y_FORWARD)),
            far_away(jnp.asarray(X_FORWARD)),
        ),
        [kept(2, 46), table_scratch, table_scratch, pltpu.SemaphoreType.DMA((2,))],
    )
    columns = exchanged(spectrum.reshape(CHIPS, 8 * DEEP, N))
    columns = run(
        column_kernel,
        f32(8 * N, N),
        [in_vmem] * 4,
        (columns.reshape(8 * N, N), influence, Z_FORWARD, Z_INVERSE),
        mib=8,
    )
    levels = exchanged(columns.reshape(CHIPS, 8 * DEEP, N))
    part = f32(3, PAIR, HERE)
    mine, for_near, for_same, for_cross, sums = run(
        sample_kernel,
        (part, part, part, part, f32(SLABS, N)),
        [in_vmem] * 7,
        (levels.reshape(CHIPS, DEEP, 8, N), own, near, same, cross, X_INVERSE, Y_INVERSE),
        [
            kept(4, 40),
            pltpu.VMEM((4, 3, PAIR, HERE), jnp.float32),
            pltpu.VMEM((2 * PAIR, LANES), jnp.float32),
        ],
    )
    from_near = moved(for_near, TO_PARTNER, back=True)
    from_same = moved(for_same, UP_SAME, back=True)
    from_cross = moved(for_cross, UP_CROSS, back=True)
    sums = lax.all_to_all(sums.reshape(SLABS, 1, N), "slab", 0, 0, tiled=True)
    return pl.pallas_call(
        finish_kernel,
        out_shape=(f32(3, WINDOWS, HERE), f32(WINDOWS), f32(WINDOWS)),
        in_specs=[in_vmem] * 5,
        out_specs=(in_vmem, in_smem, in_smem),
        compiler_params=pltpu.CompilerParams(vmem_limit_bytes=4 << 20),
        name="finish_kernel",
    )(mine, from_near, from_same, from_cross, sums.reshape(SLABS, N))


def solution(mesh):
    return jax.shard_map(
        body,
        mesh=mesh,
        in_specs=(
            P("win"),
            P("win", "slab"),
            P("win", "slab"),
            P("win", "slab"),
            P(None, "win", "slab"),
            P(None, None, "win", "slab"),
            P(None, None, "win", "slab"),
        ),
        out_specs=(P(None, "win", "slab"), P("win"), P("win")),
        check_vma=False,
    )
```
